256 devices in a mesh: field: 16 (over y_hi, z), gx: 4 (over x), gy: 4 (over y_lo, core).
Axes of the slice: x: 4, y: 4 (y_hi: 2, y_lo: 2; y = y_hi * 2 + y_lo), z: 8, core: 2. Of those that a mesh axis runs over, the one named last changes fastest.
Arguments:
- concentrations: float32 [16, 16, 16, 32, 128], P('field', None, 'gx', 'gy'), may hold values from 0 to 2
- velocity: float32 [3, 16, 32, 128], P(None, 'gx', 'gy'), may hold values from -0.3 to 0.3
- diffusivity: float32 [16, 32, 128], P('gx', 'gy'), may hold values from 0.02 to 0.12
- wiener: float32 [2, 3, 16, 16, 32, 128], P(None, None, 'field', 'gx', 'gy'), may hold values from -1.8 to 1.8
- mix_rate: float32 [16, 32, 128], P('gx', 'gy'), may hold values from 0.2 to 2
- rate_constants: float32 [64], replicated, may hold values from 0.1 to 1
- reactions: int32 [64, 4], replicated, may hold values from 0 to 15
Outputs:
- advanced: float32 [16, 16, 16, 32, 128], P('field', None, 'gx', 'gy')
The draws below stay inside these ranges and needn't reach their ends.
Inputs may be any that keep to these rules, and one draw needn't show every extreme that they name: `reactions`: each row names two reactant and two product scalars.
All inputs are finite; a program needn't handle non-finite values.
Results may differ from the reference program's by a relative error of at most 0.0001.
Values sent between devices are 32-bit elements; how exact they have to be, the bound alone decides.
A program may use at most 64 MiB of HBM per device.

```python
import math
import jax
import jax.numpy as jnp
from jax import lax

NS = 16
NR = 64
SUBSTEPS = 12
STEPS = 2
FIELDS = 16
NX = 16
NY = 32
NZ = 128


def plant(values, stream_key, least, top_value):
    extent = values.shape
    place = [jax.random.randint(jax.random.fold_in(stream_key, axis), (), 0, extent[axis]) for axis in range(len(extent))]
    values = values.at[tuple(place)].set(least)
    longest = extent.index(max(extent))
    place[longest] = (place[longest] + 1) % extent[longest]
    return values.at[tuple(place)].set(top_value)


def shard_levels(stream_key, shape, pieces, low, high):
    factor_of = 1.0
    for dim, parts in pieces:
        draws = jax.random.uniform(jax.random.fold_in(jax.random.fold_in(stream_key, 6), dim), (parts,), jnp.float32, low / len(pieces), high / len(pieces))
        factor_of = factor_of * jnp.repeat(jnp.exp(draws), shape[dim] // parts).reshape((-1,) + (1,) * (len(shape) - 1 - dim))
    return factor_of


def scatter_about(key, dims, scale, bound, cuts=(), kind=jnp.bfloat16):
    array = scale * jax.random.normal(key, dims, jnp.float32)
    if cuts:
        array = array * shard_levels(key, dims, cuts, -0.22, 0.18)
    return jnp.clip(array, -bound, bound).astype(kind)


def setup_inputs(seed: int = 0) -> dict:
    seeds = jax.random.split(jax.random.key(seed), 8)
    concentrations = jnp.clip(2.0 * jax.random.uniform(seeds[0], (FIELDS, NS, NX, NY, NZ), jnp.float32) ** shard_levels(seeds[0], (FIELDS, NS, NX, NY, NZ), ((0, 16), (2, 4), (3, 4)), -0.2, 0.2), 0.0, 2.0)
    velocity = jnp.clip(jax.random.uniform(seeds[1], (3, NX, NY, NZ), jnp.float32, -0.3, 0.3) * shard_levels(seeds[1], (3, NX, NY, NZ), ((1, 4), (2, 4)), -0.4, 0.0), -0.3, 0.3)
    diffusivity = jnp.clip(0.02 + 0.09999999776482582 * jax.random.uniform(seeds[2], (NX, NY, NZ), jnp.float32) ** shard_levels(seeds[2], (NX, NY, NZ), ((0, 4), (1, 4)), -0.2, 0.2), 0.02, 0.12)
    wiener = scatter_about(seeds[3], (STEPS, 3, FIELDS, NX, NY, NZ), 0.3, 1.8, ((2, 16), (3, 4), (4, 4)), jnp.float32)
    mix_rate = jnp.clip(jnp.exp(math.log(2.0) - 2.3025851 * jax.random.uniform(seeds[4], (NX, NY, NZ), jnp.float32) ** shard_levels(seeds[4], (NX, NY, NZ), ((0, 4), (1, 4)), -0.2, 0.2)), 0.2, 2.0)
    rate_constants = jnp.clip(jnp.exp(jax.random.uniform(seeds[5], (NR,), jnp.float32, math.log(0.1), math.log(1.0))), 0.1, 1.0)
    reactions = plant(jax.random.randint(seeds[6], (NR, 4), 0, NS), jax.random.fold_in(seeds[6], 1), 0, NS - 1).astype(jnp.int32)
    return {"concentrations": concentrations, "velocity": velocity, "diffusivity": diffusivity, "wiener": wiener, "mix_rate": mix_rate, "rate_constants": rate_constants, "reactions": reactions}


chem_step = 0.04
highest = lax.Precision.HIGHEST

def tables(reactions, count):
    scalar_ids = jnp.arange(count, dtype=jnp.int32)[None, :]
    react = (reactions[:, 0:1] == scalar_ids).astype(jnp.float32) + (reactions[:, 1:2] == scalar_ids).astype(jnp.float32)
    produce = (reactions[:, 2:3] == scalar_ids).astype(jnp.float32) + (reactions[:, 3:4] == scalar_ids).astype(jnp.float32)
    return (react, (produce - react).T)

def neighbours(values):
    middle = (slice(1, -1), slice(1, -1), slice(1, -1))
    leading = (slice(None),) * (values.ndim - 3)
    result = []
    for dim_index in range(3):
        upper_cut = list(middle)
        upper_cut[dim_index] = slice(2, None)
        lower_cut = list(middle)
        lower_cut[dim_index] = slice(0, -2)
        result.append((values[leading + tuple(upper_cut)], values[leading + tuple(lower_cut)]))
    return result

def transport(padded, gamma_pad, gamma, velocity, increments):
    centre = padded[:, 1:-1, 1:-1, 1:-1]
    pairs = neighbours(padded)
    gamma_pairs = neighbours(gamma_pad)
    noise_amp = jnp.sqrt(2.0 * gamma)
    change = jnp.zeros_like(centre)
    for dim_index in range(3):
        upward, downward = pairs[dim_index]
        gamma_up, gamma_down = gamma_pairs[dim_index]
        change = change + 0.5 * (gamma + gamma_up) * (upward - centre) + 0.5 * (gamma + gamma_down) * (downward - centre)
        change = change + (noise_amp * increments[dim_index] - velocity[dim_index]) * (0.5 * (upward - downward))
    return centre + change

def chemistry(values, react, net_t, rate_constants):

    def substep(index, conc):
        logs = jnp.log(jax.nn.softplus(conc))
        flux = rate_constants[:, None] * jnp.exp(jnp.dot(react, logs, precision=highest))
        return conc + chem_step * jnp.dot(net_t, flux, precision=highest)
    return lax.fori_loop(0, SUBSTEPS, substep, values)

def closure(first, second, count, mix_rate):
    mean = first / count
    meansq = second / count
    spread = lax.optimization_barrier(jnp.sum(meansq - mean * mean, axis=0))
    energy = lax.optimization_barrier(jnp.sum(meansq, axis=0))
    omega = mix_rate * (1.0 + spread / (1.0 + energy))
    return (mean, jnp.exp(-0.5 * omega))

def reference(concentrations, velocity, diffusivity, wiener, mix_rate, rate_constants, reactions):
    react, net_t = tables(reactions, NS)
    gamma_pad = jnp.pad(diffusivity, 1)
    conc = concentrations
    for step_index in range(STEPS):

        def advance(pair):
            field_conc, increments = pair
            padded = jnp.pad(field_conc, ((0, 0), (1, 1), (1, 1), (1, 1)))
            moved = transport(padded, gamma_pad, diffusivity, velocity, increments)
            flat = chemistry(moved.reshape(NS, -1), react, net_t, rate_constants)
            return flat.reshape(moved.shape)
        conc = lax.map(advance, (conc, jnp.moveaxis(wiener[step_index], 1, 0)))
        first = lax.optimization_barrier(jnp.sum(conc, axis=0))
        second = lax.optimization_barrier(jnp.sum(conc * conc, axis=0))
        mean, decay = closure(first, second, FIELDS, mix_rate)
        conc = mean + (conc - mean) * decay
    return conc
```

```python
import functools

import jax
import jax.numpy as jnp
import numpy as np
from jax import lax
from jax.experimental import pallas as pl
from jax.experimental.pallas import tpu as pltpu
from jax.sharding import PartitionSpec as P

SUBSTEPS = 12
STEPS = 2
DT = 0.04
LOG2E = 1.4426950408889634
LN2 = 0.6931471805599453
f32 = jnp.float32
bf16 = jnp.bfloat16
MESH = pl.DeviceIdType.MESH


def split2(x):
    hi = x.astype(bf16)
    return hi, (x - hi.astype(f32)).astype(bf16)


def make_weights(reac, k_row, w1, w2):
    nr, ns = reac.shape[0], w2.shape[0]
    ids = lax.broadcasted_iota(jnp.int32, (nr, ns), 1)

    def one_hot(j):
        return (reac[:, j : j + 1] == ids).astype(f32)

    react = one_hot(0) + one_hot(1)
    net = one_hot(2) + one_hot(3) - react
    eye = lax.broadcasted_iota(jnp.int32, (nr, nr), 0) == lax.broadcasted_iota(
        jnp.int32, (nr, nr), 1
    )
    k_col = jnp.sum(jnp.where(eye, jnp.broadcast_to(k_row, (nr, nr)), 0.0), axis=1, keepdims=True)
    bias = jnp.log(k_col * (DT * LOG2E)) * LOG2E + 2.0 * float(np.log2(LN2))
    b0 = bias.astype(bf16).astype(f32)
    b1 = (bias - b0).astype(bf16).astype(f32)
    b2 = bias - b0 - b1
    cols = jnp.where(ids == 0, b0, jnp.where(ids == 1, b1, jnp.where(ids == 2, b2, 0.0)))
    w1[...] = jnp.concatenate([react, react, cols], axis=1).astype(bf16)
    net_t = net.T
    w2[...] = jnp.concatenate([net_t, net_t], axis=1).astype(bf16)


def log2_softplus(y):
    e = jnp.exp2(-jnp.abs(y))
    big = jnp.log(1.0 + e) * LOG2E
    small = e * (LOG2E - (0.5 * LOG2E) * e)
    s = jnp.maximum(y, 0.0) + jnp.where(e < 1e-4, small, big)
    return jnp.log(s) * LOG2E


def substep(y, w1, w2):
    hi, lo = split2(log2_softplus(y))
    ones = jnp.ones((16, y.shape[1]), bf16)
    x = jnp.concatenate([hi, lo, ones], axis=0)
    flux = jnp.exp2(jnp.dot(w1[...], x, preferred_element_type=f32))
    fh, fl = split2(flux)
    return y + jnp.dot(w2[...], jnp.concatenate([fh, fl], axis=0), preferred_element_type=f32)


def kernel(
    sizes,
    conc, vel, gam, wie, mix, rate, reac,
    out,
    pad, gxr, gyr, gys, gpad, coef, ybuf, w1, w2, share, energy,
    got_s, got_e, mean, decay,
    hs_send, hs_recv, g_send, g_recv, rs_send, rs_recv, ag_send, ag_recv,
):
    nf, ngx, ngy = sizes
    ns, lx, ly, lz = conc.shape[1:]
    per = lx * ly // nf
    me = lax.axis_index("field")
    gx = lax.axis_index("gx")
    gy = lax.axis_index("gy")
    has = {
        ("gx", 0): gx > 0,
        ("gx", 1): gx < ngx - 1,
        ("gy", 0): gy > 0,
        ("gy", 1): gy < ngy - 1,
    }
    at = {
        ("gx", 0): gx - 1,
        ("gx", 1): gx + 1,
        ("gy", 0): gy - 1,
        ("gy", 1): gy + 1,
    }
    sides = [("gx", 0), ("gx", 1), ("gy", 0), ("gy", 1)]

    barrier = pltpu.get_barrier_semaphore()
    for k in range(1, nf):
        pl.semaphore_signal(
            barrier, inc=1, device_id={"field": lax.rem(me + k, nf)}, device_id_type=MESH
        )
    for side in sides:

        @pl.when(has[side])
        def _(side=side):
            pl.semaphore_signal(barrier, inc=1, device_id={side[0]: at[side]}, device_id_type=MESH)

    neighbours = sum(has[s].astype(jnp.int32) for s in sides)

    for x in range(lx):
        pad[0, x + 1, 1 : ly + 1] = jnp.swapaxes(conc[0, :, x], 0, 1)
    for i in range(2):
        gys[i] = gam[:, (ly - 1) * i, :]
    zero_x = jnp.zeros((ly, ns, lz), f32)
    zero_y = jnp.zeros((lx, ns, lz), f32)
    for axis, i in sides:

        @pl.when(jnp.logical_not(has[axis, i]))
        def _(axis=axis, i=i):
            if axis == "gx":
                gxr[i] = jnp.zeros((ly, lz), f32)
                for step in range(STEPS):
                    pad[step, (lx + 1) * i, 1 : ly + 1] = zero_x
            else:
                gyr[i] = jnp.zeros((lx, lz), f32)
                for step in range(STEPS):
                    pad[step, 1 : lx + 1, (ly + 1) * i] = zero_y

    make_weights(reac[...], rate[...].reshape(1, -1), w1, w2)

    pl.semaphore_wait(barrier, neighbours + (nf - 1))

    def face_copy(step, n):
        axis, i = sides[n]
        if axis == "gx":
            src = pad.at[step, lx if i else 1, pl.ds(1, ly)]
            dst = pad.at[step, 0 if i else lx + 1, pl.ds(1, ly)]
        else:
            src = pad.at[step, pl.ds(1, lx), ly if i else 1]
            dst = pad.at[step, pl.ds(1, lx), 0 if i else ly + 1]
        m = n ^ 1
        return pltpu.make_async_remote_copy(
            src, dst, hs_send.at[step, n], hs_recv.at[step, m],
            device_id={axis: at[axis, i]}, device_id_type=MESH,
        )

    def face_arrival(step, n):
        axis, i = sides[n]
        if axis == "gx":
            dst = pad.at[step, (lx + 1) * i, pl.ds(1, ly)]
        else:
            dst = pad.at[step, pl.ds(1, lx), (ly + 1) * i]
        return pltpu.make_async_copy(dst, dst, hs_recv.at[step, n])

    def gamma_copy(n):
        axis, i = sides[n]
        if axis == "gx":
            src, dst = gam.at[(lx - 1) * i], gxr.at[1 - i]
        else:
            src, dst = gys.at[i], gyr.at[1 - i]
        return pltpu.make_async_remote_copy(
            src, dst, g_send.at[n], g_recv.at[n ^ 1],
            device_id={axis: at[axis, i]}, device_id_type=MESH,
        )

    def gamma_arrival(n):
        axis, i = sides[n]
        dst = gxr.at[i] if axis == "gx" else gyr.at[i]
        return pltpu.make_async_copy(dst, dst, g_recv.at[n])

    def for_sides(f):
        for n in range(4):
            pl.when(has[sides[n]])(functools.partial(f, n))

    def start_faces(step):
        for_sides(lambda n: face_copy(step, n).start())

    start_faces(0)
    for_sides(lambda n: gamma_copy(n).start())
    for_sides(lambda n: gamma_arrival(n).wait())

    lane = lax.broadcasted_iota(jnp.int32, (lx, ly, lz), 2)
    g = gam[...]
    gpad[0, 1 : ly + 1] = gxr[0]
    gpad[lx + 1, 1 : ly + 1] = gxr[1]
    gpad[1 : lx + 1, 1 : ly + 1] = g
    gpad[1 : lx + 1, 0] = gyr[0]
    gpad[1 : lx + 1, ly + 1] = gyr[1]
    first, last = lane == 0, lane == lz - 1
    up = [
        gpad[2 : lx + 2, 1 : ly + 1],
        gpad[1 : lx + 1, 2 : ly + 2],
        jnp.where(last, 0.0, pltpu.roll(g, lz - 1, 2)),
    ]
    down = [
        gpad[0:lx, 1 : ly + 1],
        gpad[1 : lx + 1, 0:ly],
        jnp.where(first, 0.0, pltpu.roll(g, 1, 2)),
    ]
    noise = jnp.sqrt(2.0 * g)
    centre = 1.0
    diff = []
    for d in range(3):
        a, b = 0.5 * (g + up[d]), 0.5 * (g + down[d])
        centre = centre - a - b
        diff.append((a, b))
    for step in range(STEPS):
        coef[step, 0] = centre
        for d in range(3):
            w = 0.5 * (noise * wie[step, d, 0] - vel[d])
            a, b = diff[d][0] + w, diff[d][1] - w
            if d == 2:
                a, b = jnp.where(last, 0.0, a), jnp.where(first, 0.0, b)
            coef[step, 1 + 2 * d] = a
            coef[step, 2 + 2 * d] = b

    for step in range(STEPS):
        for_sides(lambda n, step=step: face_arrival(step, n).wait())
        for x in range(lx):
            p = pad[step, x + 1, 1 : ly + 1]
            near = [
                p,
                pad[step, x + 2, 1 : ly + 1],
                pad[step, x, 1 : ly + 1],
                pad[step, x + 1, 2 : ly + 2],
                pad[step, x + 1, 0:ly],
                pltpu.roll(p, lz - 1, 2),
                pltpu.roll(p, 1, 2),
            ]
            total = 0.0
            for i, value in enumerate(near):
                total = total + value * coef[step, i, x][:, None, :]
            total = total * LOG2E
            for y in range(ly):
                ybuf[:, (x * ly + y) * lz : (x * ly + y + 1) * lz] = total[y]

        def chem(_, carry):
            ybuf[...] = substep(ybuf[...], w1, w2)
            return carry

        lax.fori_loop(0, SUBSTEPS, chem, 0)

        for c in range(lx * ly):
            r = ybuf[:, c * lz : (c + 1) * lz] * LN2
            share[step, c // per, c % per] = r
            energy[step, c // per, c % per : c % per + 1] = jnp.sum(r * r, axis=0, keepdims=True)

        def sum_copies(k, step=step):
            to = lax.rem(me + k, nf)
            slot = nf - 1 - k
            return [
                pltpu.make_async_remote_copy(
                    src.at[step, to], dst.at[step, slot],
                    rs_send.at[step, j, k], rs_recv.at[step, j, slot],
                    device_id={"field": to}, device_id_type=MESH,
                )
                for j, (src, dst) in enumerate(((share, got_s), (energy, got_e)))
            ]

        for k in range(1, nf):
            for copy in sum_copies(k):
                copy.start()
        total_s = share[step, me]
        total_e = energy[step, me]
        for k in range(1, nf):
            for copy in sum_copies(k):
                copy.wait_recv()
            total_s = total_s + got_s[step, nf - 1 - k]
            total_e = total_e + got_e[step, nf - 1 - k]
        m = total_s * (1.0 / nf)
        power = total_e * (1.0 / nf)
        spread = power - jnp.sum(m * m, axis=1)
        row = pl.multiple_of(lax.rem(me * per, ly), per)
        omega = mix[(me * per) // ly, pl.ds(row, per), :] * (1.0 + spread / (1.0 + power))
        mean[step, me] = m
        decay[step, me] = jnp.exp(-0.5 * omega)

        def mean_copies(k, step=step):
            to = lax.rem(me + k, nf)
            return [
                pltpu.make_async_remote_copy(
                    ref.at[step, me], ref.at[step, me],
                    ag_send.at[step, j, k], ag_recv.at[step, j, nf - k],
                    device_id={"field": to}, device_id_type=MESH,
                )
                for j, ref in enumerate((mean, decay))
            ]

        def mean_arrivals(k, step=step):
            owner = lax.rem(me + k, nf)
            return [
                pltpu.make_async_copy(
                    ref.at[step, owner], ref.at[step, owner], ag_recv.at[step, j, k]
                )
                for j, ref in enumerate((mean, decay))
            ]

        for k in range(1, nf):
            for copy in mean_copies(k):
                copy.start()
        for k in range(1, nf):
            for copy in mean_arrivals(k):
                copy.wait()

        for x in range(lx):
            planes = []
            for y in range(ly):
                c = x * ly + y
                m = mean[step, c // per, c % per]
                d = decay[step, c // per, c % per : c % per + 1]
                v = m + (share[step, c // per, c % per] - m) * d
                if step + 1 < STEPS:
                    pad[step + 1, x + 1, y + 1] = v
                else:
                    planes.append(v)
            if planes:
                out[0, :, x] = jnp.swapaxes(jnp.stack(planes), 0, 1)
        if step + 1 < STEPS:
            start_faces(step + 1)

        for k in range(1, nf):
            for copy in sum_copies(k) + mean_copies(k):
                copy.wait_send()

    for step in range(STEPS):
        for_sides(lambda n, step=step: face_copy(step, n).wait_send())
    for_sides(lambda n: gamma_copy(n).wait_send())


def on_device(nf, ngx, ngy, *args):
    conc = args[0]
    ns, lx, ly, lz = conc.shape[1:]
    nr = args[6].shape[0]
    per = lx * ly // nf
    vmem, dma = pltpu.VMEM, pltpu.SemaphoreType.DMA
    return pl.pallas_call(
        functools.partial(kernel, (nf, ngx, ngy)),
        out_shape=jax.ShapeDtypeStruct(conc.shape, f32),
        in_specs=[pl.BlockSpec(memory_space=pltpu.VMEM)] * 7,
        out_specs=pl.BlockSpec(memory_space=pltpu.VMEM),
        scratch_shapes=[
            vmem((STEPS, lx + 2, ly + 2, ns, lz), f32),
            vmem((2, ly, lz), f32),
            vmem((2, lx, lz), f32),
            vmem((2, lx, lz), f32),
            vmem((lx + 2, ly + 8, lz), f32),
            vmem((STEPS, 7, lx, ly, lz), f32),
            vmem((ns, lx * ly * lz), f32),
            vmem((nr, 2 * ns + 16), bf16),
            vmem((ns, 2 * nr), bf16),
            vmem((STEPS, nf, per, ns, lz), f32),
            vmem((STEPS, nf, per, lz), f32),
            vmem((STEPS, nf - 1, per, ns, lz), f32),
            vmem((STEPS, nf - 1, per, lz), f32),
            vmem((STEPS, nf, per, ns, lz), f32),
            vmem((STEPS, nf, per, lz), f32),
            dma((STEPS, 4)),
            dma((STEPS, 4)),
            dma((4,)),
            dma((4,)),
            dma((STEPS, 2, nf)),
            dma((STEPS, 2, nf)),
            dma((STEPS, 2, nf)),
            dma((STEPS, 2, nf)),
        ],
        compiler_params=pltpu.CompilerParams(collective_id=0, has_side_effects=True),
        name="combustor",
    )(*args)


def solution(mesh):
    nf, ngx, ngy = (mesh.shape[a] for a in ("field", "gx", "gy"))
    return jax.shard_map(
        functools.partial(on_device, nf, ngx, ngy),
        mesh=mesh,
        in_specs=(
            P("field", None, "gx", "gy", None),
            P(None, "gx", "gy", None),
            P("gx", "gy", None),
            P(None, None, "field", "gx", "gy", None),
            P("gx", "gy", None),
            P(),
            P(),
        ),
        out_specs=P("field", None, "gx", "gy", None),
        check_vma=False,
    )
```

```python
import functools

import jax
import jax.numpy as jnp
import numpy as np
from jax import lax
from jax.experimental import pallas as pl
from jax.experimental.pallas import tpu as pltpu
from jax.sharding import PartitionSpec as P

SUBSTEPS = 12
STEPS = 2
DT = 0.04
TILE = 256
UNROLL = 12
LOG2E = 1.4426950408889634
LN2 = 0.6931471805599453
f32 = jnp.float32
bf16 = jnp.bfloat16
MESH = pl.DeviceIdType.MESH


def split2(x):
    hi = x.astype(bf16)
    return hi, (x - hi.astype(f32)).astype(bf16)


def make_weights(reac, k_row, w1, w2):
    nr, ns = reac.shape[1], w2.shape[0]
    ids = lax.broadcasted_iota(jnp.int32, (nr, ns), 1)
    scalar = lax.broadcasted_iota(jnp.int32, (ns, nr), 0)

    def one_hot(j):
        return (reac[j : j + 1] == scalar).astype(f32)

    react_t = one_hot(0) + one_hot(1)
    net_t = one_hot(2) + one_hot(3) - react_t
    react = react_t.T
    eye = lax.broadcasted_iota(jnp.int32, (nr, nr), 0) == lax.broadcasted_iota(
        jnp.int32, (nr, nr), 1
    )
    k_col = jnp.sum(jnp.where(eye, jnp.broadcast_to(k_row, (nr, nr)), 0.0), axis=1, keepdims=True)
    bias = jnp.log(k_col * (DT * LOG2E)) * LOG2E + 2.0 * float(np.log2(LN2))
    b0 = bias.astype(bf16).astype(f32)
    b1 = (bias - b0).astype(bf16).astype(f32)
    b2 = bias - b0 - b1
    cols = jnp.where(ids == 0, b0, jnp.where(ids == 1, b1, jnp.where(ids == 2, b2, 0.0)))
    w1[...] = jnp.concatenate([react, react, cols], axis=1).astype(bf16)
    w2[...] = jnp.concatenate([net_t, net_t], axis=1).astype(bf16)


def log2_softplus(y):
    e = jnp.exp2(-jnp.abs(y))
    big = jnp.log(1.0 + e) * LOG2E
    small = e * (LOG2E - (0.5 * LOG2E) * e)
    s = jnp.maximum(y, 0.0) + jnp.where(e < 1e-4, small, big)
    return jnp.log(s) * LOG2E


def substep(y, w1, w2):
    hi, lo = split2(log2_softplus(y))
    ones = jnp.ones((16, y.shape[1]), bf16)
    x = jnp.concatenate([hi, lo, ones], axis=0)
    flux = jnp.exp2(jnp.dot(w1, x, preferred_element_type=f32))
    fh, fl = split2(flux)
    return y + jnp.dot(w2, jnp.concatenate([fh, fl], axis=0), preferred_element_type=f32)


def kernel(
    sizes,
    conc, vel, gam, wie, mix, rate, reac,
    out,
    pad, gxr, gyr, gys, gpad, coef, ybuf, w1, w2, share, energy,
    got_s, got_e, mean, decay,
    hs_send, hs_recv, g_send, g_recv, rs_send, rs_recv, ag_send, ag_recv,
):
    nf, ngx, ngy = sizes
    ns, lx, ly, lz = conc.shape[1:]
    per = lx * ly // nf
    me = lax.axis_index("field")
    gx = lax.axis_index("gx")
    gy = lax.axis_index("gy")
    has = {
        ("gx", 0): gx > 0,
        ("gx", 1): gx < ngx - 1,
        ("gy", 0): gy > 0,
        ("gy", 1): gy < ngy - 1,
    }
    at = {
        ("gx", 0): gx - 1,
        ("gx", 1): gx + 1,
        ("gy", 0): gy - 1,
        ("gy", 1): gy + 1,
    }
    sides = [("gx", 0), ("gx", 1), ("gy", 0), ("gy", 1)]

    nz = nf // 2
    offsets = [(a, b) for a in range(2) for b in range(nz) if a or b]
    offsets.sort(key=lambda o: (-(2 * o[0] + min(o[1], nz - o[1])), o[1]))
    back = [offsets.index((a, (nz - b) % nz)) for a, b in offsets]
    high, low = me // nz, lax.rem(me, nz)
    peers = [lax.rem(high + a, 2) * nz + lax.rem(low + b, nz) for a, b in offsets]
    barrier = pltpu.get_barrier_semaphore()
    for to in peers:
        pl.semaphore_signal(barrier, inc=1, device_id={"field": to}, device_id_type=MESH)
    for side in sides:

        @pl.when(has[side])
        def _(side=side):
            pl.semaphore_signal(barrier, inc=1, device_id={side[0]: at[side]}, device_id_type=MESH)

    neighbours = sum(has[s].astype(jnp.int32) for s in sides)

    for x in range(lx):
        pad[0, x + 1, 1 : ly + 1] = jnp.swapaxes(conc[0, :, x], 0, 1)
    for i in range(2):
        gys[i] = gam[:, (ly - 1) * i, :]
    zero_x = jnp.zeros((ly, ns, lz), f32)
    zero_y = jnp.zeros((lx, ns, lz), f32)
    for axis, i in sides:

        @pl.when(jnp.logical_not(has[axis, i]))
        def _(axis=axis, i=i):
            if axis == "gx":
                gxr[i] = jnp.zeros((ly, lz), f32)
                for step in range(STEPS):
                    pad[step, (lx + 1) * i, 1 : ly + 1] = zero_x
            else:
                gyr[i] = jnp.zeros((lx, lz), f32)
                for step in range(STEPS):
                    pad[step, 1 : lx + 1, (ly + 1) * i] = zero_y

    make_weights(reac[...], rate[...].reshape(1, -1), w1, w2)

    pl.semaphore_wait(barrier, neighbours + (nf - 1))

    def face_copy(step, n):
        axis, i = sides[n]
        if axis == "gx":
            src = pad.at[step, lx if i else 1, pl.ds(1, ly)]
            dst = pad.at[step, 0 if i else lx + 1, pl.ds(1, ly)]
        else:
            src = pad.at[step, pl.ds(1, lx), ly if i else 1]
            dst = pad.at[step, pl.ds(1, lx), 0 if i else ly + 1]
        m = n ^ 1
        return pltpu.make_async_remote_copy(
            src, dst, hs_send.at[step, n], hs_recv.at[step, m],
            device_id={axis: at[axis, i]}, device_id_type=MESH,
        )

    def face_arrival(step, n):
        axis, i = sides[n]
        if axis == "gx":
            dst = pad.at[step, (lx + 1) * i, pl.ds(1, ly)]
        else:
            dst = pad.at[step, pl.ds(1, lx), (ly + 1) * i]
        return pltpu.make_async_copy(dst, dst, hs_recv.at[step, n])

    def gamma_copy(n):
        axis, i = sides[n]
        if axis == "gx":
            src, dst = gam.at[(lx - 1) * i], gxr.at[1 - i]
        else:
            src, dst = gys.at[i], gyr.at[1 - i]
        return pltpu.make_async_remote_copy(
            src, dst, g_send.at[n], g_recv.at[n ^ 1],
            device_id={axis: at[axis, i]}, device_id_type=MESH,
        )

    def gamma_arrival(n):
        axis, i = sides[n]
        dst = gxr.at[i] if axis == "gx" else gyr.at[i]
        return pltpu.make_async_copy(dst, dst, g_recv.at[n])

    def for_sides(f):
        for n in range(4):
            pl.when(has[sides[n]])(functools.partial(f, n))

    def start_faces(step):
        for_sides(lambda n: face_copy(step, n).start())

    start_faces(0)
    for_sides(lambda n: gamma_copy(n).start())
    for_sides(lambda n: gamma_arrival(n).wait())

    lane = lax.broadcasted_iota(jnp.int32, (lx, ly, lz), 2)
    g = gam[...]
    gpad[0, 1 : ly + 1] = gxr[0]
    gpad[lx + 1, 1 : ly + 1] = gxr[1]
    gpad[1 : lx + 1, 1 : ly + 1] = g
    gpad[1 : lx + 1, 0] = gyr[0]
    gpad[1 : lx + 1, ly + 1] = gyr[1]
    first, last = lane == 0, lane == lz - 1
    up = [
        gpad[2 : lx + 2, 1 : ly + 1],
        gpad[1 : lx + 1, 2 : ly + 2],
        jnp.where(last, 0.0, pltpu.roll(g, lz - 1, 2)),
    ]
    down = [
        gpad[0:lx, 1 : ly + 1],
        gpad[1 : lx + 1, 0:ly],
        jnp.where(first, 0.0, pltpu.roll(g, 1, 2)),
    ]
    noise = jnp.sqrt(2.0 * g)
    centre = 1.0
    diff = []
    for d in range(3):
        a, b = 0.5 * (g + up[d]), 0.5 * (g + down[d])
        centre = centre - a - b
        diff.append((a, b))
    for step in range(STEPS):
        coef[step, 0] = centre
        for d in range(3):
            w = 0.5 * (noise * wie[step, d, 0] - vel[d])
            a, b = diff[d][0] + w, diff[d][1] - w
            if d == 2:
                a, b = jnp.where(last, 0.0, a), jnp.where(first, 0.0, b)
            coef[step, 1 + 2 * d] = a
            coef[step, 2 + 2 * d] = b

    for step in range(STEPS):
        for_sides(lambda n, step=step: face_arrival(step, n).wait())
        for x in range(lx):
            p = pad[step, x + 1, 1 : ly + 1]
            near = [
                p,
                pad[step, x + 2, 1 : ly + 1],
                pad[step, x, 1 : ly + 1],
                pad[step, x + 1, 2 : ly + 2],
                pad[step, x + 1, 0:ly],
                pltpu.roll(p, lz - 1, 2),
                pltpu.roll(p, 1, 2),
            ]
            total = 0.0
            for i, value in enumerate(near):
                total = total + value * coef[step, i, x][:, None, :]
            total = total * LOG2E
            for y in range(ly):
                ybuf[:, (x * ly + y) * lz : (x * ly + y + 1) * lz] = total[y]

        def chem(_, carry):
            a, b = w1[...], w2[...]
            ys = [ybuf[:, q * TILE : (q + 1) * TILE] for q in range(lx * ly * lz // TILE)]
            for _ in range(UNROLL):
                ys = [substep(y, a, b) for y in ys]
            for q, y in enumerate(ys):
                ybuf[:, q * TILE : (q + 1) * TILE] = y
            return carry

        lax.fori_loop(0, SUBSTEPS // UNROLL, chem, 0)

        for c in range(lx * ly):
            r = ybuf[:, c * lz : (c + 1) * lz] * LN2
            share[step, c // per, c % per] = r
            energy[step, c // per, c % per : c % per + 1] = jnp.sum(r * r, axis=0, keepdims=True)

        def sum_copies(k, step=step):
            to, slot = peers[k], back[k]
            return [
                pltpu.make_async_remote_copy(
                    src.at[step, to], dst.at[step, slot],
                    rs_send.at[step, j, k], rs_recv.at[step, j, slot],
                    device_id={"field": to}, device_id_type=MESH,
                )
                for j, (src, dst) in enumerate(((share, got_s), (energy, got_e)))
            ]

        for k in range(nf - 1):
            for copy in sum_copies(k):
                copy.start()
        total_s = share[step, me]
        total_e = energy[step, me]
        for k in range(nf - 1):
            for copy in sum_copies(k):
                copy.wait_recv()
            total_s = total_s + got_s[step, back[k]]
            total_e = total_e + got_e[step, back[k]]
        m = total_s * (1.0 / nf)
        power = total_e * (1.0 / nf)
        spread = power - jnp.sum(m * m, axis=1)
        row = pl.multiple_of(lax.rem(me * per, ly), per)
        omega = mix[(me * per) // ly, pl.ds(row, per), :] * (1.0 + spread / (1.0 + power))
        mean[step, me] = m
        decay[step, me] = jnp.exp(-0.5 * omega)

        def mean_copies(k, step=step):
            to = peers[k]
            return [
                pltpu.make_async_remote_copy(
                    ref.at[step, me], ref.at[step, me],
                    ag_send.at[step, j, k], ag_recv.at[step, j, back[k]],
                    device_id={"field": to}, device_id_type=MESH,
                )
                for j, ref in enumerate((mean, decay))
            ]

        def mean_arrivals(k, step=step):
            owner = peers[k]
            return [
                pltpu.make_async_copy(
                    ref.at[step, owner], ref.at[step, owner], ag_recv.at[step, j, k]
                )
                for j, ref in enumerate((mean, decay))
            ]

        for k in range(nf - 1):
            for copy in mean_copies(k):
                copy.start()
        for k in range(nf - 1):
            for copy in mean_arrivals(k):
                copy.wait()

        for x in range(lx):
            planes = []
            for y in range(ly):
                c = x * ly + y
                m = mean[step, c // per, c % per]
                d = decay[step, c // per, c % per : c % per + 1]
                v = m + (share[step, c // per, c % per] - m) * d
                if step + 1 < STEPS:
                    pad[step + 1, x + 1, y + 1] = v
                else:
                    planes.append(v)
            if planes:
                out[0, :, x] = jnp.swapaxes(jnp.stack(planes), 0, 1)
        if step + 1 < STEPS:
            start_faces(step + 1)

        for k in range(nf - 1):
            for copy in sum_copies(k) + mean_copies(k):
                copy.wait_send()

    for step in range(STEPS):
        for_sides(lambda n, step=step: face_copy(step, n).wait_send())
    for_sides(lambda n: gamma_copy(n).wait_send())


def on_device(nf, ngx, ngy, *args):
    conc = args[0]
    ns, lx, ly, lz = conc.shape[1:]
    args = (*args[:6], args[6].T)
    nr = args[6].shape[1]
    per = lx * ly // nf
    vmem, dma = pltpu.VMEM, pltpu.SemaphoreType.DMA
    return pl.pallas_call(
        functools.partial(kernel, (nf, ngx, ngy)),
        out_shape=jax.ShapeDtypeStruct(conc.shape, f32),
        in_specs=[pl.BlockSpec(memory_space=pltpu.VMEM)] * 7,
        out_specs=pl.BlockSpec(memory_space=pltpu.VMEM),
        scratch_shapes=[
            vmem((STEPS, lx + 2, ly + 2, ns, lz), f32),
            vmem((2, ly, lz), f32),
            vmem((2, lx, lz), f32),
            vmem((2, lx, lz), f32),
            vmem((lx + 2, ly + 8, lz), f32),
            vmem((STEPS, 7, lx, ly, lz), f32),
            vmem((ns, lx * ly * lz), f32),
            vmem((nr, 2 * ns + 16), bf16),
            vmem((ns, 2 * nr), bf16),
            vmem((STEPS, nf, per, ns, lz), f32),
            vmem((STEPS, nf, per, lz), f32),
            vmem((STEPS, nf - 1, per, ns, lz), f32),
            vmem((STEPS, nf - 1, per, lz), f32),
            vmem((STEPS, nf, per, ns, lz), f32),
            vmem((STEPS, nf, per, lz), f32),
            dma((STEPS, 4)),
            dma((STEPS, 4)),
            dma((4,)),
            dma((4,)),
            dma((STEPS, 2, nf)),
            dma((STEPS, 2, nf)),
            dma((STEPS, 2, nf)),
            dma((STEPS, 2, nf)),
        ],
        compiler_params=pltpu.CompilerParams(collective_id=0, has_side_effects=True),
        name="combustor",
    )(*args)


def solution(mesh):
    nf, ngx, ngy = (mesh.shape[a] for a in ("field", "gx", "gy"))
    return jax.shard_map(
        functools.partial(on_device, nf, ngx, ngy),
        mesh=mesh,
        in_specs=(
            P("field", None, "gx", "gy", None),
            P(None, "gx", "gy", None),
            P("gx", "gy", None),
            P(None, None, "field", "gx", "gy", None),
            P("gx", "gy", None),
            P(),
            P(),
        ),
        out_specs=P("field", None, "gx", "gy", None),
        check_vma=False,
    )
```

```python
import functools

import jax
import jax.numpy as jnp
import numpy as np
from jax import lax
from jax.experimental import pallas as pl
from jax.experimental.pallas import tpu as pltpu
from jax.sharding import PartitionSpec as P

SUBSTEPS = 12
STEPS = 2
DT = 0.04
TILE = 256
AHEAD = (3, 10)
LOG2E = 1.4426950408889634
LN2 = 0.6931471805599453
f32 = jnp.float32
bf16 = jnp.bfloat16
MESH = pl.DeviceIdType.MESH


def split2(x):
    hi = x.astype(bf16)
    return hi, (x - hi.astype(f32)).astype(bf16)


def make_weights(reac, k_row, w1, w2):
    nr, ns = reac.shape[1], w2.shape[0]
    ids = lax.broadcasted_iota(jnp.int32, (nr, ns), 1)
    scalar = lax.broadcasted_iota(jnp.int32, (ns, nr), 0)

    def one_hot(j):
        return (reac[j : j + 1] == scalar).astype(f32)

    react_t = one_hot(0) + one_hot(1)
    net_t = one_hot(2) + one_hot(3) - react_t
    react = react_t.T
    eye = lax.broadcasted_iota(jnp.int32, (nr, nr), 0) == lax.broadcasted_iota(
        jnp.int32, (nr, nr), 1
    )
    k_col = jnp.sum(jnp.where(eye, jnp.broadcast_to(k_row, (nr, nr)), 0.0), axis=1, keepdims=True)
    bias = jnp.log(k_col * (DT * LOG2E)) * LOG2E + 2.0 * float(np.log2(LN2))
    b0 = bias.astype(bf16).astype(f32)
    b1 = (bias - b0).astype(bf16).astype(f32)
    b2 = bias - b0 - b1
    cols = jnp.where(ids == 0, b0, jnp.where(ids == 1, b1, jnp.where(ids == 2, b2, 0.0)))
    w1[...] = jnp.concatenate([react, react, cols], axis=1).astype(bf16)
    w2[...] = jnp.concatenate([net_t, net_t], axis=1).astype(bf16)


def log2_softplus(y):
    e = jnp.exp2(-jnp.abs(y))
    big = jnp.log(1.0 + e) * LOG2E
    small = e * (LOG2E - (0.5 * LOG2E) * e)
    s = jnp.maximum(y, 0.0) + jnp.where(e < 1e-4, small, big)
    return jnp.log(s) * LOG2E


def substep(y, w1, w2):
    hi, lo = split2(log2_softplus(y))
    ones = jnp.ones((16, y.shape[1]), bf16)
    x = jnp.concatenate([hi, lo, ones], axis=0)
    flux = jnp.exp2(jnp.dot(w1, x, preferred_element_type=f32))
    fh, fl = split2(flux)
    return y + jnp.dot(w2, jnp.concatenate([fh, fl], axis=0), preferred_element_type=f32)


def kernel(
    sizes,
    conc_h, vel_h, gam_h, wie_h, mix_h, rate_h, reac_h,
    out,
    conc, vel, gam, wie, mix, rate, reac, in_sem,
    pad, gxr, gyr, gys, gpad, coef, ybuf, w1, w2, share, got, mean,
    hs_send, hs_recv, g_send, g_recv, rs_send, rs_recv, ag_send, ag_recv,
):
    nf, ngx, ngy = sizes
    ns, lx, ly, lz = conc.shape[1:]
    planes = [list(range(1, lx - 1)), [0, lx - 1]]
    chunks = [[(x, y) for x in xs for y in range(ly)] for xs in planes]
    me = lax.axis_index("field")
    gx = lax.axis_index("gx")
    gy = lax.axis_index("gy")
    has = {
        ("gx", 0): gx > 0,
        ("gx", 1): gx < ngx - 1,
        ("gy", 0): gy > 0,
        ("gy", 1): gy < ngy - 1,
    }
    at = {
        ("gx", 0): gx - 1,
        ("gx", 1): gx + 1,
        ("gy", 0): gy - 1,
        ("gy", 1): gy + 1,
    }
    sides = [("gx", 0), ("gx", 1), ("gy", 0), ("gy", 1)]

    nz = nf // 2
    offsets = [(a, b) for a in range(2) for b in range(nz) if a or b]
    offsets.sort(key=lambda o: (-(2 * o[0] + min(o[1], nz - o[1])), o[1]))
    back = [offsets.index((a, (nz - b) % nz)) for a, b in offsets]
    high, low = me // nz, lax.rem(me, nz)
    peers = [lax.rem(high + a, 2) * nz + lax.rem(low + b, nz) for a, b in offsets]
    barrier = pltpu.get_barrier_semaphore()
    for to in peers:
        pl.semaphore_signal(barrier, inc=1, device_id={"field": to}, device_id_type=MESH)
    for side in sides:

        @pl.when(has[side])
        def _(side=side):
            pl.semaphore_signal(barrier, inc=1, device_id={side[0]: at[side]}, device_id_type=MESH)

    neighbours = sum(has[s].astype(jnp.int32) for s in sides)

    loads = [
        pltpu.make_async_copy(a, b, in_sem.at[i])
        for i, (a, b) in enumerate(
            (
                (conc_h, conc), (gam_h, gam), (reac_h, reac), (rate_h, rate),
                (wie_h, wie), (vel_h, vel), (mix_h, mix),
            )
        )
    ]
    for load in loads:
        load.start()
    for load in loads[:2]:
        load.wait()
    for x in range(lx):
        pad[0, x + 1, 1 : ly + 1] = jnp.swapaxes(conc[0, :, x], 0, 1)
    for i in range(2):
        gys[i] = gam[:, (ly - 1) * i, :]
    zero_x = jnp.zeros((ly, ns, lz), f32)
    zero_y = jnp.zeros((lx, ns, lz), f32)
    for axis, i in sides:

        @pl.when(jnp.logical_not(has[axis, i]))
        def _(axis=axis, i=i):
            if axis == "gx":
                gxr[i] = jnp.zeros((ly, lz), f32)
                for step in range(STEPS):
                    pad[step, (lx + 1) * i, 1 : ly + 1] = zero_x
            else:
                gyr[i] = jnp.zeros((lx, lz), f32)
                for step in range(STEPS):
                    pad[step, 1 : lx + 1, (ly + 1) * i] = zero_y

    for load in loads[2:]:
        load.wait()
    make_weights(reac[...], rate[...].reshape(1, -1), w1, w2)

    pl.semaphore_wait(barrier, neighbours + (nf - 1))

    pieces = [(n, p) for n in range(4) for p in ((0,) if n < 2 else (0, 1, 2))]
    of_chunk = [[q for q in pieces if q[1] == 2], [q for q in pieces if q[1] < 2]]

    def face(step, n, p, inside):
        axis, i = sides[n]
        if axis == "gx":
            x = (lx if i else 1) if inside else (lx + 1) * i
            return pad.at[step, x, pl.ds(1, ly)]
        y = (ly if i else 1) if inside else (ly + 1) * i
        if p == 2:
            return pad.at[step, pl.ds(2, lx - 2), y]
        return pad.at[step, lx if p else 1, y]

    def face_copy(step, n, p):
        axis, i = sides[n]
        return pltpu.make_async_remote_copy(
            face(step, n, p, True), face(step, n ^ 1, p, False),
            hs_send.at[step, n, p], hs_recv.at[step, n ^ 1, p],
            device_id={axis: at[axis, i]}, device_id_type=MESH,
        )

    def face_arrival(step, n, p):
        dst = face(step, n, p, False)
        return pltpu.make_async_copy(dst, dst, hs_recv.at[step, n, p])

    def gamma_copy(n):
        axis, i = sides[n]
        if axis == "gx":
            src, dst = gam.at[(lx - 1) * i], gxr.at[1 - i]
        else:
            src, dst = gys.at[i], gyr.at[1 - i]
        return pltpu.make_async_remote_copy(
            src, dst, g_send.at[n], g_recv.at[n ^ 1],
            device_id={axis: at[axis, i]}, device_id_type=MESH,
        )

    def gamma_arrival(n):
        axis, i = sides[n]
        dst = gxr.at[i] if axis == "gx" else gyr.at[i]
        return pltpu.make_async_copy(dst, dst, g_recv.at[n])

    def for_sides(f):
        for n in range(4):
            pl.when(has[sides[n]])(functools.partial(f, n))

    def for_pieces(step, chosen, f):
        for n in range(4):

            @pl.when(has[sides[n]])
            def _(n=n):
                for m, p in chosen:
                    if m == n:
                        f(step, n, p)

    def start_faces(step, chosen):
        for_pieces(step, chosen, lambda *q: face_copy(*q).start())

    for_sides(lambda n: gamma_copy(n).start())
    for chosen in of_chunk:
        start_faces(0, chosen)
    for_sides(lambda n: gamma_arrival(n).wait())

    lane = lax.broadcasted_iota(jnp.int32, (lx, ly, lz), 2)
    g = gam[...]
    gpad[0, 1 : ly + 1] = gxr[0]
    gpad[lx + 1, 1 : ly + 1] = gxr[1]
    gpad[1 : lx + 1, 1 : ly + 1] = g
    gpad[1 : lx + 1, 0] = gyr[0]
    gpad[1 : lx + 1, ly + 1] = gyr[1]
    first, last = lane == 0, lane == lz - 1
    up = [
        gpad[2 : lx + 2, 1 : ly + 1],
        gpad[1 : lx + 1, 2 : ly + 2],
        jnp.where(last, 0.0, pltpu.roll(g, lz - 1, 2)),
    ]
    down = [
        gpad[0:lx, 1 : ly + 1],
        gpad[1 : lx + 1, 0:ly],
        jnp.where(first, 0.0, pltpu.roll(g, 1, 2)),
    ]
    noise = jnp.sqrt(2.0 * g)
    centre = 1.0
    diff = []
    for d in range(3):
        a, b = 0.5 * (g + up[d]), 0.5 * (g + down[d])
        centre = centre - a - b
        diff.append((a, b))
    for step in range(STEPS):
        coef[step, 0] = centre
        for d in range(3):
            w = 0.5 * (noise * wie[step, d, 0] - vel[d])
            a, b = diff[d][0] + w, diff[d][1] - w
            if d == 2:
                a, b = jnp.where(last, 0.0, a), jnp.where(first, 0.0, b)
            coef[step, 1 + 2 * d] = a
            coef[step, 2 + 2 * d] = b

    for step in range(STEPS):
        def move(chunk, step=step):
            for x in planes[chunk]:
                p = pad[step, x + 1, 1 : ly + 1]
                near = [
                    p,
                    pad[step, x + 2, 1 : ly + 1],
                    pad[step, x, 1 : ly + 1],
                    pad[step, x + 1, 2 : ly + 2],
                    pad[step, x + 1, 0:ly],
                    pltpu.roll(p, lz - 1, 2),
                    pltpu.roll(p, 1, 2),
                ]
                total = 0.0
                for i, value in enumerate(near):
                    total = total + value * coef[step, i, x][:, None, :]
                total = total * LOG2E
                for y in range(ly):
                    ybuf[:, (x * ly + y) * lz : (x * ly + y + 1) * lz] = total[y]

        def react(which, count):
            a, b = w1[...], w2[...]
            starts = [
                i for c in which for x in planes[c] for i in range(x * ly * lz, (x + 1) * ly * lz, TILE)
            ]
            ys = [ybuf[:, i : i + TILE] for i in starts]
            for _ in range(count):
                ys = [substep(y, a, b) for y in ys]
            for i, y in zip(starts, ys):
                ybuf[:, i : i + TILE] = y

        def sum_copy(c, k, step=step):
            return pltpu.make_async_remote_copy(
                share.at[step, c, peers[k]], got.at[step, c, back[k]],
                rs_send.at[step, c, k], rs_recv.at[step, c, back[k]],
                device_id={"field": peers[k]}, device_id_type=MESH,
            )

        def mean_copy(c, k, step=step):
            return pltpu.make_async_remote_copy(
                mean.at[step, c, me], mean.at[step, c, me],
                ag_send.at[step, c, k], ag_recv.at[step, c, back[k]],
                device_id={"field": peers[k]}, device_id_type=MESH,
            )

        def publish(c, step=step):
            for o, (x, y) in enumerate(chunks[c]):
                at_cell = (x * ly + y) * lz
                r = ybuf[:, at_cell : at_cell + lz] * LN2
                share[step, c, o, 0:ns] = r
                share[step, c, o, ns : ns + 1] = jnp.sum(r * r, axis=0, keepdims=True)
            for k in range(nf - 1):
                sum_copy(c, k).start()

        for_pieces(step, of_chunk[0], lambda *q: face_arrival(*q).wait())
        move(0)
        react((0,), AHEAD[step])
        for_pieces(step, of_chunk[1], lambda *q: face_arrival(*q).wait())
        move(1)
        react((0, 1), SUBSTEPS - AHEAD[step])
        publish(0)
        react((1,), AHEAD[step])
        publish(1)

        for c in range(2):
            total = share[step, c, me]
            for k in range(nf - 1):
                sum_copy(c, k).wait_recv()
                total = total + got[step, c, back[k]]
            total = total * (1.0 / nf)
            m, power = total[0:ns], total[ns : ns + 1]
            spread = power - jnp.sum(m * m, axis=0, keepdims=True)
            x, y = me // ly, lax.rem(me, ly)
            x = x * (lx - 1) if c else x + 1
            omega = mix[x, pl.ds(y, 1), :] * (1.0 + spread / (1.0 + power))
            mean[step, c, me, 0:ns] = m
            mean[step, c, me, ns : ns + 1] = jnp.exp(-0.5 * omega)
            for k in range(nf - 1):
                mean_copy(c, k).start()

        for c, cells in enumerate(chunks):
            for k in range(nf - 1):
                pltpu.make_async_copy(
                    mean.at[step, c, peers[k]], mean.at[step, c, peers[k]], ag_recv.at[step, c, k]
                ).wait()
            for o, (x, y) in enumerate(cells):
                m = mean[step, c, o, 0:ns]
                v = m + (share[step, c, o, 0:ns] - m) * mean[step, c, o, ns : ns + 1]
                if step + 1 < STEPS:
                    pad[step + 1, x + 1, y + 1] = v
                else:
                    ybuf[:, (x * ly + y) * lz : (x * ly + y + 1) * lz] = v
            if step + 1 < STEPS:
                start_faces(step + 1, of_chunk[c])
        if step + 1 == STEPS:
            for x in range(lx):
                rows = [
                    ybuf[:, (x * ly + y) * lz : (x * ly + y + 1) * lz] for y in range(ly)
                ]
                out[0, :, x] = jnp.swapaxes(jnp.stack(rows), 0, 1)
        for c in range(2):
            for k in range(nf - 1):
                sum_copy(c, k).wait_send()
                mean_copy(c, k).wait_send()
    for step in range(STEPS):
        for_pieces(step, pieces, lambda *q: face_copy(*q).wait_send())
    for_sides(lambda n: gamma_copy(n).wait_send())


def on_device(nf, ngx, ngy, *args):
    conc = args[0]
    ns, lx, ly, lz = conc.shape[1:]
    args = (*args[:6], args[6].T)
    nr = args[6].shape[1]
    vmem, dma = pltpu.VMEM, pltpu.SemaphoreType.DMA
    return pl.pallas_call(
        functools.partial(kernel, (nf, ngx, ngy)),
        out_shape=jax.ShapeDtypeStruct(conc.shape, f32),
        in_specs=[pl.BlockSpec(memory_space=pltpu.HBM)] * 7,
        out_specs=pl.BlockSpec(memory_space=pltpu.VMEM),
        scratch_shapes=[
            *[vmem(a.shape, a.dtype) for a in args],
            dma((7,)),
            vmem((STEPS, lx + 2, ly + 2, ns, lz), f32),
            vmem((2, ly, lz), f32),
            vmem((2, lx, lz), f32),
            vmem((2, lx, lz), f32),
            vmem((lx + 2, ly + 8, lz), f32),
            vmem((STEPS, 7, lx, ly, lz), f32),
            vmem((ns, lx * ly * lz), f32),
            vmem((nr, 2 * ns + 16), bf16),
            vmem((ns, 2 * nr), bf16),
            vmem((STEPS, 2, nf, ns + 1, lz), f32),
            vmem((STEPS, 2, nf - 1, ns + 1, lz), f32),
            vmem((STEPS, 2, nf, ns + 1, lz), f32),
            dma((STEPS, 4, 3)),
            dma((STEPS, 4, 3)),
            dma((4,)),
            dma((4,)),
            dma((STEPS, 2, nf)),
            dma((STEPS, 2, nf)),
            dma((STEPS, 2, nf)),
            dma((STEPS, 2, nf)),
        ],
        compiler_params=pltpu.CompilerParams(collective_id=0, has_side_effects=True),
        name="combustor",
    )(*args)


def solution(mesh):
    nf, ngx, ngy = (mesh.shape[a] for a in ("field", "gx", "gy"))
    return jax.shard_map(
        functools.partial(on_device, nf, ngx, ngy),
        mesh=mesh,
        in_specs=(
            P("field", None, "gx", "gy", None),
            P(None, "gx", "gy", None),
            P("gx", "gy", None),
            P(None, None, "field", "gx", "gy", None),
            P("gx", "gy", None),
            P(),
            P(),
        ),
        out_specs=P("field", None, "gx", "gy", None),
        check_vma=False,
    )
```

```python
import functools

import jax
import jax.numpy as jnp
import numpy as np
from jax import lax
from jax.experimental import pallas as pl
from jax.experimental.pallas import tpu as pltpu
from jax.sharding import PartitionSpec as P

SUBSTEPS = 12
STEPS = 2
DT = 0.04
TILE = 256
AHEAD = (3, 10)
LOG2E = 1.4426950408889634
LN2 = 0.6931471805599453
f32 = jnp.float32
bf16 = jnp.bfloat16
MESH = pl.DeviceIdType.MESH


def split2(x):
    hi = x.astype(bf16)
    return hi, (x - hi.astype(f32)).astype(bf16)


def make_weights(reac, k_row, w1, w2):
    nr, ns = reac.shape[1], w2.shape[0]
    ids = lax.broadcasted_iota(jnp.int32, (nr, ns), 1)
    scalar = lax.broadcasted_iota(jnp.int32, (ns, nr), 0)

    def one_hot(j):
        return (reac[j : j + 1] == scalar).astype(f32)

    react_t = one_hot(0) + one_hot(1)
    net_t = one_hot(2) + one_hot(3) - react_t
    react = react_t.T
    eye = lax.broadcasted_iota(jnp.int32, (nr, nr), 0) == lax.broadcasted_iota(
        jnp.int32, (nr, nr), 1
    )
    k_col = jnp.sum(jnp.where(eye, jnp.broadcast_to(k_row, (nr, nr)), 0.0), axis=1, keepdims=True)
    bias = jnp.log(k_col * (DT * LOG2E)) * LOG2E + 2.0 * float(np.log2(LN2))
    b0 = bias.astype(bf16).astype(f32)
    b1 = (bias - b0).astype(bf16).astype(f32)
    b2 = bias - b0 - b1
    cols = jnp.where(ids == 0, b0, jnp.where(ids == 1, b1, jnp.where(ids == 2, b2, 0.0)))
    w1[...] = jnp.concatenate([react, react, cols], axis=1).astype(bf16)
    w2[...] = jnp.concatenate([net_t, net_t], axis=1).astype(bf16)


def log2_softplus(y):
    e = jnp.exp2(-jnp.abs(y))
    big = jnp.log(1.0 + e) * LOG2E
    small = e * (LOG2E - (0.5 * LOG2E) * e)
    s = jnp.maximum(y, 0.0) + jnp.where(e < 1e-4, small, big)
    return jnp.log(s) * LOG2E


def substep(y, w1, w2):
    hi, lo = split2(log2_softplus(y))
    ones = jnp.ones((16, y.shape[1]), bf16)
    x = jnp.concatenate([hi, lo, ones], axis=0)
    flux = jnp.exp2(jnp.dot(w1, x, preferred_element_type=f32))
    fh, fl = split2(flux)
    return y + jnp.dot(w2, jnp.concatenate([fh, fl], axis=0), preferred_element_type=f32)


def kernel(
    sizes,
    conc_h, vel_h, gam_h, wie_h, mix_h, rate_h, reac_h,
    out,
    conc, vel, gam, wie, mix, rate, reac, in_sem,
    pad, gxr, gyr, gys, gpad, coef, ybuf, w1, w2, share, got, mean,
    hs_send, hs_recv, g_send, g_recv, rs_send, rs_recv, ag_send, ag_recv,
):
    nf, ngx, ngy = sizes
    ns, lx, ly, lz = conc.shape[1:]
    planes = [list(range(1, lx - 1)), [0, lx - 1]]
    chunks = [[(x, y) for x in xs for y in range(ly)] for xs in planes]
    me = lax.axis_index("field")
    gx = lax.axis_index("gx")
    gy = lax.axis_index("gy")
    has = {
        ("gx", 0): gx > 0,
        ("gx", 1): gx < ngx - 1,
        ("gy", 0): gy > 0,
        ("gy", 1): gy < ngy - 1,
    }
    at = {
        ("gx", 0): gx - 1,
        ("gx", 1): gx + 1,
        ("gy", 0): gy - 1,
        ("gy", 1): gy + 1,
    }
    sides = [("gx", 0), ("gx", 1), ("gy", 0), ("gy", 1)]

    nz = nf // 2
    offsets = [(a, b) for a in range(2) for b in range(nz) if a or b]
    offsets.sort(key=lambda o: (-(2 * o[0] + min(o[1], nz - o[1])), o[1]))
    back = [offsets.index((a, (nz - b) % nz)) for a, b in offsets]
    high, low = me // nz, lax.rem(me, nz)
    peers = [lax.rem(high + a, 2) * nz + lax.rem(low + b, nz) for a, b in offsets]
    barrier = pltpu.get_barrier_semaphore()
    for to in peers:
        pl.semaphore_signal(barrier, inc=1, device_id={"field": to}, device_id_type=MESH)
    for side in sides:

        @pl.when(has[side])
        def _(side=side):
            pl.semaphore_signal(barrier, inc=1, device_id={side[0]: at[side]}, device_id_type=MESH)

    neighbours = sum(has[s].astype(jnp.int32) for s in sides)

    loads = [
        pltpu.make_async_copy(a, b, in_sem.at[i])
        for i, (a, b) in enumerate(
            (
                (conc_h, conc), (gam_h, gam), (reac_h, reac), (rate_h, rate),
                (wie_h, wie), (vel_h, vel), (mix_h, mix),
            )
        )
    ]
    for load in loads:
        load.start()
    for load in loads[:2]:
        load.wait()
    for x in range(lx):
        pad[0, x + 1, 1 : ly + 1] = jnp.swapaxes(conc[0, :, x], 0, 1)
    for i in range(2):
        gys[i] = gam[:, (ly - 1) * i, :]
    zero_x = jnp.zeros((ly, ns, lz), f32)
    zero_y = jnp.zeros((lx, ns, lz), f32)
    for axis, i in sides:

        @pl.when(jnp.logical_not(has[axis, i]))
        def _(axis=axis, i=i):
            if axis == "gx":
                gxr[i] = jnp.zeros((ly, lz), f32)
                for step in range(STEPS):
                    pad[step, (lx + 1) * i, 1 : ly + 1] = zero_x
            else:
                gyr[i] = jnp.zeros((lx, lz), f32)
                for step in range(STEPS):
                    pad[step, 1 : lx + 1, (ly + 1) * i] = zero_y

    for load in loads[2:]:
        load.wait()
    make_weights(reac[...], rate[...].reshape(1, -1), w1, w2)

    pl.semaphore_wait(barrier, neighbours + (nf - 1))

    pieces = [(n, p) for n in range(4) for p in ((0,) if n < 2 else (0, 1, 2))]
    of_chunk = [[q for q in pieces if q[1] == 2], [q for q in pieces if q[1] < 2]]

    def face(step, n, p, inside):
        axis, i = sides[n]
        if axis == "gx":
            x = (lx if i else 1) if inside else (lx + 1) * i
            return pad.at[step, x, pl.ds(1, ly)]
        y = (ly if i else 1) if inside else (ly + 1) * i
        if p == 2:
            return pad.at[step, pl.ds(2, lx - 2), y]
        return pad.at[step, lx if p else 1, y]

    def face_copy(step, n, p):
        axis, i = sides[n]
        return pltpu.make_async_remote_copy(
            face(step, n, p, True), face(step, n ^ 1, p, False),
            hs_send.at[step, n, p], hs_recv.at[step, n ^ 1, p],
            device_id={axis: at[axis, i]}, device_id_type=MESH,
        )

    def face_arrival(step, n, p):
        dst = face(step, n, p, False)
        return pltpu.make_async_copy(dst, dst, hs_recv.at[step, n, p])

    def gamma_copy(n):
        axis, i = sides[n]
        if axis == "gx":
            src, dst = gam.at[(lx - 1) * i], gxr.at[1 - i]
        else:
            src, dst = gys.at[i], gyr.at[1 - i]
        return pltpu.make_async_remote_copy(
            src, dst, g_send.at[n], g_recv.at[n ^ 1],
            device_id={axis: at[axis, i]}, device_id_type=MESH,
        )

    def gamma_arrival(n):
        axis, i = sides[n]
        dst = gxr.at[i] if axis == "gx" else gyr.at[i]
        return pltpu.make_async_copy(dst, dst, g_recv.at[n])

    def for_sides(f):
        for n in range(4):
            pl.when(has[sides[n]])(functools.partial(f, n))

    def for_pieces(step, chosen, f):
        for n in range(4):

            @pl.when(has[sides[n]])
            def _(n=n):
                for m, p in chosen:
                    if m == n:
                        f(step, n, p)

    def start_faces(step, chosen):
        for_pieces(step, chosen, lambda *q: face_copy(*q).start())

    for_sides(lambda n: gamma_copy(n).start())
    for chosen in of_chunk:
        start_faces(0, chosen)
    for_sides(lambda n: gamma_arrival(n).wait())

    lane = lax.broadcasted_iota(jnp.int32, (lx, ly, lz), 2)
    g = gam[...]
    gpad[0, 1 : ly + 1] = gxr[0]
    gpad[lx + 1, 1 : ly + 1] = gxr[1]
    gpad[1 : lx + 1, 1 : ly + 1] = g
    gpad[1 : lx + 1, 0] = gyr[0]
    gpad[1 : lx + 1, ly + 1] = gyr[1]
    first, last = lane == 0, lane == lz - 1
    up = [
        gpad[2 : lx + 2, 1 : ly + 1],
        gpad[1 : lx + 1, 2 : ly + 2],
        jnp.where(last, 0.0, pltpu.roll(g, lz - 1, 2)),
    ]
    down = [
        gpad[0:lx, 1 : ly + 1],
        gpad[1 : lx + 1, 0:ly],
        jnp.where(first, 0.0, pltpu.roll(g, 1, 2)),
    ]
    noise = jnp.sqrt(2.0 * g)
    centre = 1.0
    diff = []
    for d in range(3):
        a, b = 0.5 * (g + up[d]), 0.5 * (g + down[d])
        centre = centre - a - b
        diff.append((a, b))
    for step in range(STEPS):
        coef[step, 0] = centre
        for d in range(3):
            w = 0.5 * (noise * wie[step, d, 0] - vel[d])
            a, b = diff[d][0] + w, diff[d][1] - w
            if d == 2:
                a, b = jnp.where(last, 0.0, a), jnp.where(first, 0.0, b)
            coef[step, 1 + 2 * d] = a
            coef[step, 2 + 2 * d] = b

    for step in range(STEPS):
        def move(chunk, step=step):
            for x in planes[chunk]:
                p = pad[step, x + 1, 1 : ly + 1]
                near = [
                    p,
                    pad[step, x + 2, 1 : ly + 1],
                    pad[step, x, 1 : ly + 1],
                    pad[step, x + 1, 2 : ly + 2],
                    pad[step, x + 1, 0:ly],
                    pltpu.roll(p, lz - 1, 2),
                    pltpu.roll(p, 1, 2),
                ]
                total = 0.0
                for i, value in enumerate(near):
                    total = total + value * coef[step, i, x][:, None, :]
                total = total * LOG2E
                for y in range(ly):
                    ybuf[:, (x * ly + y) * lz : (x * ly + y + 1) * lz] = total[y]

        def react(which, count):
            a, b = w1[...], w2[...]
            starts = [
                i for c in which for x in planes[c] for i in range(x * ly * lz, (x + 1) * ly * lz, TILE)
            ]
            ys = [ybuf[:, i : i + TILE] for i in starts]
            for _ in range(count):
                ys = [substep(y, a, b) for y in ys]
            for i, y in zip(starts, ys):
                ybuf[:, i : i + TILE] = y

        def sum_copy(c, k, step=step):
            return pltpu.make_async_remote_copy(
                share.at[step, c, peers[k]], got.at[step, c, back[k]],
                rs_send.at[step, c, k], rs_recv.at[step, c, back[k]],
                device_id={"field": peers[k]}, device_id_type=MESH,
            )

        def mean_copy(c, k, step=step):
            return pltpu.make_async_remote_copy(
                mean.at[step, c, me], mean.at[step, c, me],
                ag_send.at[step, c, k], ag_recv.at[step, c, back[k]],
                device_id={"field": peers[k]}, device_id_type=MESH,
            )

        def publish(c, step=step):
            for o, (x, y) in enumerate(chunks[c]):
                at_cell = (x * ly + y) * lz
                r = ybuf[:, at_cell : at_cell + lz] * LN2
                share[step, c, o, 0:ns] = r
                share[step, c, o, ns : ns + 1] = jnp.sum(r * r, axis=0, keepdims=True)
            for k in range(nf - 1):
                sum_copy(c, k).start()

        for_pieces(step, of_chunk[0], lambda *q: face_arrival(*q).wait())
        move(0)
        react((0,), AHEAD[step])
        for_pieces(step, of_chunk[1], lambda *q: face_arrival(*q).wait())
        move(1)
        react((0, 1), SUBSTEPS - AHEAD[step])
        publish(0)
        react((1,), AHEAD[step])
        publish(1)

        for c in range(2):
            total = share[step, c, me]
            for k in range(nf - 1):
                sum_copy(c, k).wait_recv()
                total = total + got[step, c, back[k]]
            total = total * (1.0 / nf)
            m, power = total[0:ns], total[ns : ns + 1]
            spread = power - jnp.sum(m * m, axis=0, keepdims=True)
            x, y = me // ly, lax.rem(me, ly)
            x = x * (lx - 1) if c else x + 1
            omega = mix[x, pl.ds(y, 1), :] * (1.0 + spread / (1.0 + power))
            mean[step, c, me, 0:ns] = m
            mean[step, c, me, ns : ns + 1] = jnp.exp(-0.5 * omega)
            for k in range(nf - 1):
                mean_copy(c, k).start()

        for c, cells in enumerate(chunks):
            for k in range(nf - 1):
                pltpu.make_async_copy(
                    mean.at[step, c, peers[k]], mean.at[step, c, peers[k]], ag_recv.at[step, c, k]
                ).wait()
            for o, (x, y) in enumerate(cells):
                m = mean[step, c, o, 0:ns]
                v = m + (share[step, c, o, 0:ns] - m) * mean[step, c, o, ns : ns + 1]
                if step + 1 < STEPS:
                    pad[step + 1, x + 1, y + 1] = v
                else:
                    ybuf[:, (x * ly + y) * lz : (x * ly + y + 1) * lz] = v
            if step + 1 < STEPS:
                start_faces(step + 1, of_chunk[c])
        if step + 1 == STEPS:
            for x in range(lx):
                rows = [
                    ybuf[:, (x * ly + y) * lz : (x * ly + y + 1) * lz] for y in range(ly)
                ]
                out[0, :, x] = jnp.swapaxes(jnp.stack(rows), 0, 1)
        for c in range(2):
            for k in range(nf - 1):
                sum_copy(c, k).wait_send()
                mean_copy(c, k).wait_send()
    for step in range(STEPS):
        for_pieces(step, pieces, lambda *q: face_copy(*q).wait_send())
    for_sides(lambda n: gamma_copy(n).wait_send())


def on_device(nf, ngx, ngy, *args):
    conc = args[0]
    ns, lx, ly, lz = conc.shape[1:]
    args = tuple(pltpu.with_memory_space_constraint(a, pltpu.HBM) for a in (*args[:6], args[6].T))
    nr = args[6].shape[1]
    vmem, dma = pltpu.VMEM, pltpu.SemaphoreType.DMA
    return pl.pallas_call(
        functools.partial(kernel, (nf, ngx, ngy)),
        out_shape=jax.ShapeDtypeStruct(conc.shape, f32),
        in_specs=[pl.BlockSpec(memory_space=pltpu.HBM)] * 7,
        out_specs=pl.BlockSpec(memory_space=pltpu.VMEM),
        scratch_shapes=[
            *[vmem(a.shape, a.dtype) for a in args],
            dma((7,)),
            vmem((STEPS, lx + 2, ly + 2, ns, lz), f32),
            vmem((2, ly, lz), f32),
            vmem((2, lx, lz), f32),
            vmem((2, lx, lz), f32),
            vmem((lx + 2, ly + 8, lz), f32),
            vmem((STEPS, 7, lx, ly, lz), f32),
            vmem((ns, lx * ly * lz), f32),
            vmem((nr, 2 * ns + 16), bf16),
            vmem((ns, 2 * nr), bf16),
            vmem((STEPS, 2, nf, ns + 1, lz), f32),
            vmem((STEPS, 2, nf - 1, ns + 1, lz), f32),
            vmem((STEPS, 2, nf, ns + 1, lz), f32),
            dma((STEPS, 4, 3)),
            dma((STEPS, 4, 3)),
            dma((4,)),
            dma((4,)),
            dma((STEPS, 2, nf)),
            dma((STEPS, 2, nf)),
            dma((STEPS, 2, nf)),
            dma((STEPS, 2, nf)),
        ],
        compiler_params=pltpu.CompilerParams(collective_id=0, has_side_effects=True, vmem_limit_bytes=16777216),
        name="combustor",
    )(*args)


def solution(mesh):
    nf, ngx, ngy = (mesh.shape[a] for a in ("field", "gx", "gy"))
    return jax.shard_map(
        functools.partial(on_device, nf, ngx, ngy),
        mesh=mesh,
        in_specs=(
            P("field", None, "gx", "gy", None),
            P(None, "gx", "gy", None),
            P("gx", "gy", None),
            P(None, None, "field", "gx", "gy", None),
            P("gx", "gy", None),
            P(),
            P(),
        ),
        out_specs=P("field", None, "gx", "gy", None),
        check_vma=False,
    )
```

```python
import functools

import jax
import jax.numpy as jnp
import numpy as np
from jax import lax
from jax.experimental import pallas as pl
from jax.experimental.pallas import tpu as pltpu
from jax.sharding import PartitionSpec as P

SUBSTEPS = 12
STEPS = 2
DT = 0.04
TILE = 256
AHEAD = (3, 10)
LOG2E = 1.4426950408889634
LN2 = 0.6931471805599453
f32 = jnp.float32
bf16 = jnp.bfloat16
MESH = pl.DeviceIdType.MESH


def split2(x):
    hi = x.astype(bf16)
    return hi, (x - hi.astype(f32)).astype(bf16)


def make_weights(reac, k_row, w1, w2):
    nr, ns = reac.shape[1], w2.shape[0]
    ids = lax.broadcasted_iota(jnp.int32, (nr, ns), 1)
    scalar = lax.broadcasted_iota(jnp.int32, (ns, nr), 0)

    def one_hot(j):
        return (reac[j : j + 1] == scalar).astype(f32)

    react_t = one_hot(0) + one_hot(1)
    net_t = one_hot(2) + one_hot(3) - react_t
    react = react_t.T
    eye = lax.broadcasted_iota(jnp.int32, (nr, nr), 0) == lax.broadcasted_iota(
        jnp.int32, (nr, nr), 1
    )
    k_col = jnp.sum(jnp.where(eye, jnp.broadcast_to(k_row, (nr, nr)), 0.0), axis=1, keepdims=True)
    bias = jnp.log(k_col * (DT * LOG2E)) * LOG2E
    b0 = bias.astype(bf16).astype(f32)
    b1 = (bias - b0).astype(bf16).astype(f32)
    b2 = bias - b0 - b1
    cols = jnp.where(ids == 0, b0, jnp.where(ids == 1, b1, jnp.where(ids == 2, b2, 0.0)))
    w1[...] = jnp.concatenate([react, react, cols], axis=1).astype(bf16)
    twice = [net_t[:, i : i + 16] for i in range(0, nr, 16) for _ in range(2)]
    w2[...] = jnp.concatenate(twice, axis=1).astype(bf16)


def log2_softplus(y):
    e = jnp.exp2(-jnp.abs(y))
    s = jnp.maximum(y * LN2, 0.0) + jnp.where(e < 1e-4, e * (1.0 - 0.5 * e), jnp.log(1.0 + e))
    return jnp.log(s) * LOG2E


def substep(y, w1, w2):
    hi, lo = split2(log2_softplus(y))
    ones = jnp.ones((16, y.shape[1]), bf16)
    x = jnp.concatenate([hi, lo, ones], axis=0)
    flux = jnp.exp2(jnp.dot(w1, x, preferred_element_type=f32))
    parts = [part for i in range(0, flux.shape[0], 16) for part in split2(flux[i : i + 16])]
    return y + jnp.dot(w2, jnp.concatenate(parts, axis=0), preferred_element_type=f32)


def kernel(
    sizes,
    conc_h, vel_h, gam_h, wie_h, mix_h, rate_h, reac_h,
    out,
    conc, vel, gam, wie, mix, rate, reac, in_sem,
    pad, gxr, gyr, gys, gpad, coef, ybuf, w1, w2, share, got, mean,
    hs_send, hs_recv, g_send, g_recv, rs_send, rs_recv, ag_send, ag_recv,
):
    nf, ngx, ngy = sizes
    ns, lx, ly, lz = conc.shape[1:]
    planes = [list(range(1, lx - 1)), [0, lx - 1]]
    chunks = [[(x, y) for x in xs for y in range(ly)] for xs in planes]
    me = lax.axis_index("field")
    gx = lax.axis_index("gx")
    gy = lax.axis_index("gy")
    has = {
        ("gx", 0): gx > 0,
        ("gx", 1): gx < ngx - 1,
        ("gy", 0): gy > 0,
        ("gy", 1): gy < ngy - 1,
    }
    at = {
        ("gx", 0): gx - 1,
        ("gx", 1): gx + 1,
        ("gy", 0): gy - 1,
        ("gy", 1): gy + 1,
    }
    sides = [("gx", 0), ("gx", 1), ("gy", 0), ("gy", 1)]

    nz = nf // 2
    offsets = [(a, b) for a in range(2) for b in range(nz) if a or b]
    offsets.sort(key=lambda o: (-(2 * o[0] + min(o[1], nz - o[1])), o[1]))
    back = [offsets.index((a, (nz - b) % nz)) for a, b in offsets]
    high, low = me // nz, lax.rem(me, nz)
    peers = [lax.rem(high + a, 2) * nz + lax.rem(low + b, nz) for a, b in offsets]
    loads = [
        pltpu.make_async_copy(a, b, in_sem.at[i])
        for i, (a, b) in enumerate(
            (
                (conc_h, conc), (gam_h, gam), (reac_h, reac), (rate_h, rate),
                (wie_h, wie), (vel_h, vel), (mix_h, mix),
            )
        )
    ]
    for load in loads:
        load.start()
    barrier = pltpu.get_barrier_semaphore()
    for to in peers:
        pl.semaphore_signal(barrier, inc=1, device_id={"field": to}, device_id_type=MESH)

    for side in sides:

        @pl.when(has[side])
        def _(side=side):
            pl.semaphore_signal(barrier, inc=1, device_id={side[0]: at[side]}, device_id_type=MESH)

    neighbours = sum(has[s].astype(jnp.int32) for s in sides)

    for load in loads[:2]:
        load.wait()
    for x in range(lx):
        pad[0, x + 1, 1 : ly + 1] = jnp.swapaxes(conc[0, :, x], 0, 1)
    for i in range(2):
        gys[i] = gam[:, (ly - 1) * i, :]
    pl.semaphore_wait(barrier, neighbours + (nf - 1))

    pieces = [(n, p) for n in range(4) for p in ((0,) if n < 2 else (0, 1, 2))]
    of_chunk = [[q for q in pieces if q[1] == 2], [q for q in pieces if q[1] < 2]]

    def face(step, n, p, inside):
        axis, i = sides[n]
        if axis == "gx":
            x = (lx if i else 1) if inside else (lx + 1) * i
            return pad.at[step, x, pl.ds(1, ly)]
        y = (ly if i else 1) if inside else (ly + 1) * i
        if p == 2:
            return pad.at[step, pl.ds(2, lx - 2), y]
        return pad.at[step, lx if p else 1, y]

    def face_copy(step, n, p):
        axis, i = sides[n]
        return pltpu.make_async_remote_copy(
            face(step, n, p, True), face(step, n ^ 1, p, False),
            hs_send.at[step, n, p], hs_recv.at[step, n ^ 1, p],
            device_id={axis: at[axis, i]}, device_id_type=MESH,
        )

    def face_arrival(step, n, p):
        dst = face(step, n, p, False)
        return pltpu.make_async_copy(dst, dst, hs_recv.at[step, n, p])

    def gamma_copy(n):
        axis, i = sides[n]
        if axis == "gx":
            src, dst = gam.at[(lx - 1) * i], gxr.at[1 - i]
        else:
            src, dst = gys.at[i], gyr.at[1 - i]
        return pltpu.make_async_remote_copy(
            src, dst, g_send.at[n], g_recv.at[n ^ 1],
            device_id={axis: at[axis, i]}, device_id_type=MESH,
        )

    def gamma_arrival(n):
        axis, i = sides[n]
        dst = gxr.at[i] if axis == "gx" else gyr.at[i]
        return pltpu.make_async_copy(dst, dst, g_recv.at[n])

    def for_sides(f):
        for n in range(4):
            pl.when(has[sides[n]])(functools.partial(f, n))

    def for_pieces(step, chosen, f):
        for n in range(4):

            @pl.when(has[sides[n]])
            def _(n=n):
                for m, p in chosen:
                    if m == n:
                        f(step, n, p)

    def start_faces(step, chosen):
        for_pieces(step, chosen, lambda *q: face_copy(*q).start())

    for_sides(lambda n: gamma_copy(n).start())
    for chosen in of_chunk:
        start_faces(0, chosen)
    for load in loads[2:]:
        load.wait()
    make_weights(reac[...], rate[...].reshape(1, -1), w1, w2)

    zero_x = jnp.zeros((ly, ns, lz), f32)
    zero_y = jnp.zeros((lx, ns, lz), f32)
    for axis, i in sides:

        @pl.when(jnp.logical_not(has[axis, i]))
        def _(axis=axis, i=i):
            if axis == "gx":
                gxr[i] = jnp.zeros((ly, lz), f32)
                for step in range(STEPS):
                    pad[step, (lx + 1) * i, 1 : ly + 1] = zero_x
            else:
                gyr[i] = jnp.zeros((lx, lz), f32)
                for step in range(STEPS):
                    pad[step, 1 : lx + 1, (ly + 1) * i] = zero_y

    for_sides(lambda n: gamma_arrival(n).wait())

    lane = lax.broadcasted_iota(jnp.int32, (lx, ly, lz), 2)
    g = gam[...]
    gpad[0, 1 : ly + 1] = gxr[0]
    gpad[lx + 1, 1 : ly + 1] = gxr[1]
    gpad[1 : lx + 1, 1 : ly + 1] = g
    gpad[1 : lx + 1, 0] = gyr[0]
    gpad[1 : lx + 1, ly + 1] = gyr[1]
    first, last = lane == 0, lane == lz - 1
    up = [
        gpad[2 : lx + 2, 1 : ly + 1],
        gpad[1 : lx + 1, 2 : ly + 2],
        jnp.where(last, 0.0, pltpu.roll(g, lz - 1, 2)),
    ]
    down = [
        gpad[0:lx, 1 : ly + 1],
        gpad[1 : lx + 1, 0:ly],
        jnp.where(first, 0.0, pltpu.roll(g, 1, 2)),
    ]
    noise = jnp.sqrt(2.0 * g)
    centre = 1.0
    diff = []
    for d in range(3):
        a, b = 0.5 * (g + up[d]), 0.5 * (g + down[d])
        centre = centre - a - b
        diff.append((a, b))
    for step in range(STEPS):
        coef[step, 0] = centre
        for d in range(3):
            w = 0.5 * (noise * wie[step, d, 0] - vel[d])
            a, b = diff[d][0] + w, diff[d][1] - w
            if d == 2:
                a, b = jnp.where(last, 0.0, a), jnp.where(first, 0.0, b)
            coef[step, 1 + 2 * d] = a
            coef[step, 2 + 2 * d] = b

    for step in range(STEPS):
        def move(chunk, step=step):
            for x in planes[chunk]:
                p = pad[step, x + 1, 1 : ly + 1]
                near = [
                    p,
                    pad[step, x + 2, 1 : ly + 1],
                    pad[step, x, 1 : ly + 1],
                    pad[step, x + 1, 2 : ly + 2],
                    pad[step, x + 1, 0:ly],
                    pltpu.roll(p, lz - 1, 2),
                    pltpu.roll(p, 1, 2),
                ]
                total = 0.0
                for i, value in enumerate(near):
                    total = total + value * coef[step, i, x][:, None, :]
                total = total * LOG2E
                for y in range(ly):
                    ybuf[:, (x * ly + y) * lz : (x * ly + y + 1) * lz] = total[y]

        def react(which, count):
            a, b = w1[...], w2[...]
            starts = [
                i for c in which for x in planes[c] for i in range(x * ly * lz, (x + 1) * ly * lz, TILE)
            ]
            ys = [ybuf[:, i : i + TILE] for i in starts]
            for _ in range(count):
                ys = [substep(y, a, b) for y in ys]
            for i, y in zip(starts, ys):
                ybuf[:, i : i + TILE] = y

        def sum_copy(c, k, step=step):
            return pltpu.make_async_remote_copy(
                share.at[step, c, peers[k]], got.at[step, c, back[k]],
                rs_send.at[step, c, k], rs_recv.at[step, c, back[k]],
                device_id={"field": peers[k]}, device_id_type=MESH,
            )

        def mean_copy(c, k, step=step):
            return pltpu.make_async_remote_copy(
                mean.at[step, c, me], mean.at[step, c, me],
                ag_send.at[step, c, k], ag_recv.at[step, c, back[k]],
                device_id={"field": peers[k]}, device_id_type=MESH,
            )

        def publish(c, step=step):
            for o, (x, y) in enumerate(chunks[c]):
                at_cell = (x * ly + y) * lz
                r = ybuf[:, at_cell : at_cell + lz] * LN2
                share[step, c, o, 0:ns] = r
                share[step, c, o, ns : ns + 1] = jnp.sum(r * r, axis=0, keepdims=True)
            for k in range(nf - 1):
                sum_copy(c, k).start()

        for_pieces(step, of_chunk[0], lambda *q: face_arrival(*q).wait())
        move(0)
        react((0,), AHEAD[step])
        for_pieces(step, of_chunk[1], lambda *q: face_arrival(*q).wait())
        move(1)
        react((0, 1), SUBSTEPS - AHEAD[step])
        publish(0)
        react((1,), AHEAD[step])
        publish(1)

        for c in range(2):
            total = share[step, c, me]
            for k in reversed(range(nf - 1)):
                sum_copy(c, k).wait_recv()
                total = total + got[step, c, back[k]]
            total = total * (1.0 / nf)
            m, power = total[0:ns], total[ns : ns + 1]
            spread = power - jnp.sum(m * m, axis=0, keepdims=True)
            x, y = me // ly, lax.rem(me, ly)
            x = x * (lx - 1) if c else x + 1
            omega = mix[x, pl.ds(y, 1), :] * (1.0 + spread / (1.0 + power))
            mean[step, c, me, 0:ns] = m
            mean[step, c, me, ns : ns + 1] = jnp.exp(-0.5 * omega)
            for k in range(nf - 1):
                mean_copy(c, k).start()

        for c, cells in enumerate(chunks):
            for k in reversed(range(nf - 1)):
                pltpu.make_async_copy(
                    mean.at[step, c, peers[k]], mean.at[step, c, peers[k]], ag_recv.at[step, c, k]
                ).wait()
            for o, (x, y) in enumerate(cells):
                m = mean[step, c, o, 0:ns]
                v = m + (share[step, c, o, 0:ns] - m) * mean[step, c, o, ns : ns + 1]
                if step + 1 < STEPS:
                    pad[step + 1, x + 1, y + 1] = v
                else:
                    ybuf[:, (x * ly + y) * lz : (x * ly + y + 1) * lz] = v
            if step + 1 < STEPS:
                start_faces(step + 1, of_chunk[c])
        if step + 1 == STEPS:
            for x in range(lx):
                rows = [
                    ybuf[:, (x * ly + y) * lz : (x * ly + y + 1) * lz] for y in range(ly)
                ]
                out[0, :, x] = jnp.swapaxes(jnp.stack(rows), 0, 1)
        for c in range(2):
            for k in range(nf - 1):
                sum_copy(c, k).wait_send()
                mean_copy(c, k).wait_send()
    for step in range(STEPS):
        for_pieces(step, pieces, lambda *q: face_copy(*q).wait_send())
    for_sides(lambda n: gamma_copy(n).wait_send())


def on_device(nf, ngx, ngy, *args):
    conc = args[0]
    ns, lx, ly, lz = conc.shape[1:]
    args = tuple(pltpu.with_memory_space_constraint(a, pltpu.HBM) for a in (*args[:6], args[6].T))
    nr = args[6].shape[1]
    vmem, dma = pltpu.VMEM, pltpu.SemaphoreType.DMA
    return pl.pallas_call(
        functools.partial(kernel, (nf, ngx, ngy)),
        out_shape=jax.ShapeDtypeStruct(conc.shape, f32),
        in_specs=[pl.BlockSpec(memory_space=pltpu.HBM)] * 7,
        out_specs=pl.BlockSpec(memory_space=pltpu.VMEM),
        scratch_shapes=[
            *[vmem(a.shape, a.dtype) for a in args],
            dma((7,)),
            vmem((STEPS, lx + 2, ly + 2, ns, lz), f32),
            vmem((2, ly, lz), f32),
            vmem((2, lx, lz), f32),
            vmem((2, lx, lz), f32),
            vmem((lx + 2, ly + 8, lz), f32),
            vmem((STEPS, 7, lx, ly, lz), f32),
            vmem((ns, lx * ly * lz), f32),
            vmem((nr, 2 * ns + 16), bf16),
            vmem((ns, 2 * nr), bf16),
            vmem((STEPS, 2, nf, ns + 1, lz), f32),
            vmem((STEPS, 2, nf - 1, ns + 1, lz), f32),
            vmem((STEPS, 2, nf, ns + 1, lz), f32),
            dma((STEPS, 4, 3)),
            dma((STEPS, 4, 3)),
            dma((4,)),
            dma((4,)),
            dma((STEPS, 2, nf)),
            dma((STEPS, 2, nf)),
            dma((STEPS, 2, nf)),
            dma((STEPS, 2, nf)),
        ],
        compiler_params=pltpu.CompilerParams(collective_id=0, has_side_effects=True, vmem_limit_bytes=16777216),
        name="combustor",
    )(*args)


def solution(mesh):
    nf, ngx, ngy = (mesh.shape[a] for a in ("field", "gx", "gy"))
    return jax.shard_map(
        functools.partial(on_device, nf, ngx, ngy),
        mesh=mesh,
        in_specs=(
            P("field", None, "gx", "gy", None),
            P(None, "gx", "gy", None),
            P("gx", "gy", None),
            P(None, None, "field", "gx", "gy", None),
            P("gx", "gy", None),
            P(),
            P(),
        ),
        out_specs=P("field", None, "gx", "gy", None),
        check_vma=False,
    )
```

```python
import functools

import jax
import jax.numpy as jnp
import numpy as np
from jax import lax
from jax.experimental import pallas as pl
from jax.experimental.pallas import tpu as pltpu
from jax.sharding import PartitionSpec as P

SUBSTEPS = 12
STEPS = 2
DT = 0.04
TILE = 256
AHEAD = (6, 10)
LOG2E = 1.4426950408889634
LN2 = 0.6931471805599453
f32 = jnp.float32
bf16 = jnp.bfloat16
MESH = pl.DeviceIdType.MESH


def split2(x):
    hi = x.astype(bf16)
    return hi, (x - hi.astype(f32)).astype(bf16)


def make_weights(reac, k_row, w1, w2):
    nr, ns = reac.shape[1], w2.shape[0]
    ids = lax.broadcasted_iota(jnp.int32, (nr, ns), 1)
    scalar = lax.broadcasted_iota(jnp.int32, (ns, nr), 0)

    def one_hot(j):
        return (reac[j : j + 1] == scalar).astype(f32)

    react_t = one_hot(0) + one_hot(1)
    net_t = one_hot(2) + one_hot(3) - react_t
    react = react_t.T
    eye = lax.broadcasted_iota(jnp.int32, (nr, nr), 0) == lax.broadcasted_iota(
        jnp.int32, (nr, nr), 1
    )
    k_col = jnp.sum(jnp.where(eye, jnp.broadcast_to(k_row, (nr, nr)), 0.0), axis=1, keepdims=True)
    bias = jnp.log(k_col * (DT * LOG2E)) * LOG2E
    b0 = bias.astype(bf16).astype(f32)
    b1 = (bias - b0).astype(bf16).astype(f32)
    b2 = bias - b0 - b1
    cols = jnp.where(ids == 0, b0, jnp.where(ids == 1, b1, jnp.where(ids == 2, b2, 0.0)))
    w1[...] = jnp.concatenate([react, react, cols], axis=1).astype(bf16)
    twice = [net_t[:, i : i + 16] for i in range(0, nr, 16) for _ in range(2)]
    w2[...] = jnp.concatenate(twice, axis=1).astype(bf16)


def log2_softplus(y):
    e = jnp.exp2(-jnp.abs(y))
    s = jnp.maximum(y * LN2, 0.0) + jnp.where(e < 1e-4, e * (1.0 - 0.5 * e), jnp.log(1.0 + e))
    return jnp.log(s) * LOG2E


def substep(y, w1, w2):
    hi, lo = split2(log2_softplus(y))
    ones = jnp.ones((16, y.shape[1]), bf16)
    x = jnp.concatenate([hi, lo, ones], axis=0)
    flux = jnp.exp2(jnp.dot(w1, x, preferred_element_type=f32))
    parts = [part for i in range(0, flux.shape[0], 16) for part in split2(flux[i : i + 16])]
    return y + jnp.dot(w2, jnp.concatenate(parts, axis=0), preferred_element_type=f32)


def kernel(
    sizes,
    conc_h, vel_h, gam_h, wie_h, mix_h, rate_h, reac_h,
    out,
    conc, vel, gam, wie, mix, rate, reac, in_sem,
    pad, gxr, gyr, gys, gpad, coef, ybuf, w1, w2, share, got, mean,
    hs_send, hs_recv, g_send, g_recv, rs_send, rs_recv, ag_send, ag_recv,
):
    nf, ngx, ngy = sizes
    ns, lx, ly, lz = conc.shape[1:]
    planes = [list(range(1, lx - 1)), [0, lx - 1]]
    chunks = [[(x, y) for x in xs for y in range(ly)] for xs in planes]
    me = lax.axis_index("field")
    gx = lax.axis_index("gx")
    gy = lax.axis_index("gy")
    has = {
        ("gx", 0): gx > 0,
        ("gx", 1): gx < ngx - 1,
        ("gy", 0): gy > 0,
        ("gy", 1): gy < ngy - 1,
    }
    at = {
        ("gx", 0): gx - 1,
        ("gx", 1): gx + 1,
        ("gy", 0): gy - 1,
        ("gy", 1): gy + 1,
    }
    sides = [("gx", 0), ("gx", 1), ("gy", 0), ("gy", 1)]

    nz = nf // 2
    offsets = [(a, b) for a in range(2) for b in range(nz) if a or b]
    offsets.sort(key=lambda o: (-(2 * o[0] + min(o[1], nz - o[1])), o[1]))
    back = [offsets.index((a, (nz - b) % nz)) for a, b in offsets]
    high, low = me // nz, lax.rem(me, nz)
    peers = [lax.rem(high + a, 2) * nz + lax.rem(low + b, nz) for a, b in offsets]
    loads = [
        pltpu.make_async_copy(a, b, in_sem.at[i])
        for i, (a, b) in enumerate(
            (
                (conc_h, conc), (gam_h, gam), (reac_h, reac), (rate_h, rate),
                (wie_h, wie), (vel_h, vel), (mix_h, mix),
            )
        )
    ]
    for load in loads:
        load.start()
    barrier = pltpu.get_barrier_semaphore()
    for to in peers:
        pl.semaphore_signal(barrier, inc=1, device_id={"field": to}, device_id_type=MESH)

    for side in sides:

        @pl.when(has[side])
        def _(side=side):
            pl.semaphore_signal(barrier, inc=1, device_id={side[0]: at[side]}, device_id_type=MESH)

    neighbours = sum(has[s].astype(jnp.int32) for s in sides)

    for load in loads[:2]:
        load.wait()
    for x in range(lx):
        pad[0, x + 1, 1 : ly + 1] = jnp.swapaxes(conc[0, :, x], 0, 1)
    for i in range(2):
        gys[i] = gam[:, (ly - 1) * i, :]
    pl.semaphore_wait(barrier, neighbours + (nf - 1))

    pieces = [(n, p) for n in range(4) for p in ((0,) if n < 2 else (0, 1, 2))]
    of_chunk = [[q for q in pieces if q[1] == 2], [q for q in pieces if q[1] < 2]]

    def face(step, n, p, inside):
        axis, i = sides[n]
        if axis == "gx":
            x = (lx if i else 1) if inside else (lx + 1) * i
            return pad.at[step, x, pl.ds(1, ly)]
        y = (ly if i else 1) if inside else (ly + 1) * i
        if p == 2:
            return pad.at[step, pl.ds(2, lx - 2), y]
        return pad.at[step, lx if p else 1, y]

    def face_copy(step, n, p):
        axis, i = sides[n]
        return pltpu.make_async_remote_copy(
            face(step, n, p, True), face(step, n ^ 1, p, False),
            hs_send.at[step, n, p], hs_recv.at[step, n ^ 1, p],
            device_id={axis: at[axis, i]}, device_id_type=MESH,
        )

    def face_arrival(step, n, p):
        dst = face(step, n, p, False)
        return pltpu.make_async_copy(dst, dst, hs_recv.at[step, n, p])

    def gamma_copy(n):
        axis, i = sides[n]
        if axis == "gx":
            src, dst = gam.at[(lx - 1) * i], gxr.at[1 - i]
        else:
            src, dst = gys.at[i], gyr.at[1 - i]
        return pltpu.make_async_remote_copy(
            src, dst, g_send.at[n], g_recv.at[n ^ 1],
            device_id={axis: at[axis, i]}, device_id_type=MESH,
        )

    def gamma_arrival(n):
        axis, i = sides[n]
        dst = gxr.at[i] if axis == "gx" else gyr.at[i]
        return pltpu.make_async_copy(dst, dst, g_recv.at[n])

    def for_sides(f):
        for n in range(4):
            pl.when(has[sides[n]])(functools.partial(f, n))

    def for_pieces(step, chosen, f):
        for n in range(4):

            @pl.when(has[sides[n]])
            def _(n=n):
                for m, p in chosen:
                    if m == n:
                        f(step, n, p)

    def start_faces(step, chosen):
        for_pieces(step, chosen, lambda *q: face_copy(*q).start())

    for_sides(lambda n: gamma_copy(n).start())
    for chosen in of_chunk:
        start_faces(0, chosen)
    for load in loads[2:]:
        load.wait()
    make_weights(reac[...], rate[...].reshape(1, -1), w1, w2)

    zero_x = jnp.zeros((ly, ns, lz), f32)
    zero_y = jnp.zeros((lx, ns, lz), f32)
    for axis, i in sides:

        @pl.when(jnp.logical_not(has[axis, i]))
        def _(axis=axis, i=i):
            if axis == "gx":
                gxr[i] = jnp.zeros((ly, lz), f32)
                for step in range(STEPS):
                    pad[step, (lx + 1) * i, 1 : ly + 1] = zero_x
            else:
                gyr[i] = jnp.zeros((lx, lz), f32)
                for step in range(STEPS):
                    pad[step, 1 : lx + 1, (ly + 1) * i] = zero_y

    lane = lax.broadcasted_iota(jnp.int32, (ly, lz), 1)
    first, last = lane == 0, lane == lz - 1

    def coefficients(chunk):
        for x in planes[chunk]:
            g = gam[x]
            up = [
                gpad[x + 2, 1 : ly + 1],
                gpad[x + 1, 2 : ly + 2],
                jnp.where(last, 0.0, pltpu.roll(g, lz - 1, 1)),
            ]
            down = [
                gpad[x, 1 : ly + 1],
                gpad[x + 1, 0:ly],
                jnp.where(first, 0.0, pltpu.roll(g, 1, 1)),
            ]
            noise = jnp.sqrt(2.0 * g)
            centre = 1.0
            diff = []
            for d in range(3):
                a, b = 0.5 * (g + up[d]), 0.5 * (g + down[d])
                centre = centre - a - b
                diff.append((a, b))
            for step in range(STEPS):
                coef[step, 0, x] = centre
                for d in range(3):
                    w = 0.5 * (noise * wie[step, d, 0, x] - vel[d, x])
                    a, b = diff[d][0] + w, diff[d][1] - w
                    if d == 2:
                        a, b = jnp.where(last, 0.0, a), jnp.where(first, 0.0, b)
                    coef[step, 1 + 2 * d, x] = a
                    coef[step, 2 + 2 * d, x] = b

    gpad[1 : lx + 1, 1 : ly + 1] = gam[...]
    for n in (2, 3):
        pl.when(has[sides[n]])(functools.partial(lambda n: gamma_arrival(n).wait(), n))
    gpad[1 : lx + 1, 0] = gyr[0]
    gpad[1 : lx + 1, ly + 1] = gyr[1]
    coefficients(0)
    def outer_coefficients():
        for n in (0, 1):
            pl.when(has[sides[n]])(functools.partial(lambda n: gamma_arrival(n).wait(), n))
        gpad[0, 1 : ly + 1] = gxr[0]
        gpad[lx + 1, 1 : ly + 1] = gxr[1]
        coefficients(1)

    for step in range(STEPS):
        def move(chunk, step=step):
            for x in planes[chunk]:
                p = pad[step, x + 1, 1 : ly + 1]
                near = [
                    p,
                    pad[step, x + 2, 1 : ly + 1],
                    pad[step, x, 1 : ly + 1],
                    pad[step, x + 1, 2 : ly + 2],
                    pad[step, x + 1, 0:ly],
                    pltpu.roll(p, lz - 1, 2),
                    pltpu.roll(p, 1, 2),
                ]
                total = 0.0
                for i, value in enumerate(near):
                    total = total + value * coef[step, i, x][:, None, :]
                total = total * LOG2E
                for y in range(ly):
                    ybuf[:, (x * ly + y) * lz : (x * ly + y + 1) * lz] = total[y]

        def react(which, count):
            a, b = w1[...], w2[...]
            starts = [
                i for c in which for x in planes[c] for i in range(x * ly * lz, (x + 1) * ly * lz, TILE)
            ]
            ys = [ybuf[:, i : i + TILE] for i in starts]
            for _ in range(count):
                ys = [substep(y, a, b) for y in ys]
            for i, y in zip(starts, ys):
                ybuf[:, i : i + TILE] = y

        def sum_copy(c, k, step=step):
            return pltpu.make_async_remote_copy(
                share.at[step, c, peers[k]], got.at[step, c, back[k]],
                rs_send.at[step, c, k], rs_recv.at[step, c, back[k]],
                device_id={"field": peers[k]}, device_id_type=MESH,
            )

        def mean_copy(c, k, step=step):
            return pltpu.make_async_remote_copy(
                mean.at[step, c, me], mean.at[step, c, me],
                ag_send.at[step, c, k], ag_recv.at[step, c, back[k]],
                device_id={"field": peers[k]}, device_id_type=MESH,
            )

        def publish(c, step=step):
            for o, (x, y) in enumerate(chunks[c]):
                at_cell = (x * ly + y) * lz
                r = ybuf[:, at_cell : at_cell + lz] * LN2
                share[step, c, o, 0:ns] = r
                share[step, c, o, ns : ns + 1] = jnp.sum(r * r, axis=0, keepdims=True)
            for k in range(nf - 1):
                sum_copy(c, k).start()

        for_pieces(step, of_chunk[0], lambda *q: face_arrival(*q).wait())
        move(0)
        react((0,), AHEAD[step])
        if step == 0:
            outer_coefficients()
        for_pieces(step, of_chunk[1], lambda *q: face_arrival(*q).wait())
        move(1)
        react((0, 1), SUBSTEPS - AHEAD[step])
        publish(0)
        react((1,), AHEAD[step])
        publish(1)

        for c in range(2):
            total = share[step, c, me]
            for k in reversed(range(nf - 1)):
                sum_copy(c, k).wait_recv()
                total = total + got[step, c, back[k]]
            total = total * (1.0 / nf)
            m, power = total[0:ns], total[ns : ns + 1]
            spread = power - jnp.sum(m * m, axis=0, keepdims=True)
            x, y = me // ly, lax.rem(me, ly)
            x = x * (lx - 1) if c else x + 1
            omega = mix[x, pl.ds(y, 1), :] * (1.0 + spread / (1.0 + power))
            mean[step, c, me, 0:ns] = m
            mean[step, c, me, ns : ns + 1] = jnp.exp(-0.5 * omega)
            for k in range(nf - 1):
                mean_copy(c, k).start()

        for c, cells in enumerate(chunks):
            for k in reversed(range(nf - 1)):
                pltpu.make_async_copy(
                    mean.at[step, c, peers[k]], mean.at[step, c, peers[k]], ag_recv.at[step, c, k]
                ).wait()
            for o, (x, y) in enumerate(cells):
                m = mean[step, c, o, 0:ns]
                v = m + (share[step, c, o, 0:ns] - m) * mean[step, c, o, ns : ns + 1]
                if step + 1 < STEPS:
                    pad[step + 1, x + 1, y + 1] = v
                else:
                    ybuf[:, (x * ly + y) * lz : (x * ly + y + 1) * lz] = v
            if step + 1 < STEPS:
                start_faces(step + 1, of_chunk[c])
        if step + 1 == STEPS:
            for x in range(lx):
                rows = [
                    ybuf[:, (x * ly + y) * lz : (x * ly + y + 1) * lz] for y in range(ly)
                ]
                out[0, :, x] = jnp.swapaxes(jnp.stack(rows), 0, 1)
        for c in range(2):
            for k in range(nf - 1):
                sum_copy(c, k).wait_send()
                mean_copy(c, k).wait_send()
    for step in range(STEPS):
        for_pieces(step, pieces, lambda *q: face_copy(*q).wait_send())
    for_sides(lambda n: gamma_copy(n).wait_send())


def on_device(nf, ngx, ngy, *args):
    conc = args[0]
    ns, lx, ly, lz = conc.shape[1:]
    args = tuple(pltpu.with_memory_space_constraint(a, pltpu.HBM) for a in (*args[:6], args[6].T))
    nr = args[6].shape[1]
    vmem, dma = pltpu.VMEM, pltpu.SemaphoreType.DMA
    return pl.pallas_call(
        functools.partial(kernel, (nf, ngx, ngy)),
        out_shape=jax.ShapeDtypeStruct(conc.shape, f32),
        in_specs=[pl.BlockSpec(memory_space=pltpu.HBM)] * 7,
        out_specs=pl.BlockSpec(memory_space=pltpu.VMEM),
        scratch_shapes=[
            *[vmem(a.shape, a.dtype) for a in args],
            dma((7,)),
            vmem((STEPS, lx + 2, ly + 2, ns, lz), f32),
            vmem((2, ly, lz), f32),
            vmem((2, lx, lz), f32),
            vmem((2, lx, lz), f32),
            vmem((lx + 2, ly + 8, lz), f32),
            vmem((STEPS, 7, lx, ly, lz), f32),
            vmem((ns, lx * ly * lz), f32),
            vmem((nr, 2 * ns + 16), bf16),
            vmem((ns, 2 * nr), bf16),
            vmem((STEPS, 2, nf, ns + 1, lz), f32),
            vmem((STEPS, 2, nf - 1, ns + 1, lz), f32),
            vmem((STEPS, 2, nf, ns + 1, lz), f32),
            dma((STEPS, 4, 3)),
            dma((STEPS, 4, 3)),
            dma((4,)),
            dma((4,)),
            dma((STEPS, 2, nf)),
            dma((STEPS, 2, nf)),
            dma((STEPS, 2, nf)),
            dma((STEPS, 2, nf)),
        ],
        compiler_params=pltpu.CompilerParams(collective_id=0, has_side_effects=True, vmem_limit_bytes=16777216),
        name="combustor",
    )(*args)


def solution(mesh):
    nf, ngx, ngy = (mesh.shape[a] for a in ("field", "gx", "gy"))
    return jax.shard_map(
        functools.partial(on_device, nf, ngx, ngy),
        mesh=mesh,
        in_specs=(
            P("field", None, "gx", "gy", None),
            P(None, "gx", "gy", None),
            P("gx", "gy", None),
            P(None, None, "field", "gx", "gy", None),
            P("gx", "gy", None),
            P(),
            P(),
        ),
        out_specs=P("field", None, "gx", "gy", None),
        check_vma=False,
    )
```
